256 devices in a mesh: mb: 8 (over z), tp: 8 (over y, core), dp: 4 (over x).
Axes of the slice: x: 4, y: 4, z: 8, core: 2. Of those that a mesh axis runs over, the one named last changes fastest.
Arguments:
- hidden: bfloat16 [4, 16, 512, 7168], P('dp', 'mb', None, 'tp'), may hold values from -6 to 6
- latent: bfloat16 [4, 16, 512, 512], P('dp', 'mb', None, 'tp'), may hold values from -6 to 6
- out_grad: bfloat16 [4, 16, 512, 16384], P('dp', 'mb', None, 'tp'), may hold values from -0.059814453 to 0.059814453
- up_weight: bfloat16 [512, 16384], P(None, 'tp'), may hold values from -0.046875 to 0.046875
- mb_tokens: int32 [4, 16], P('dp'), may hold values from 128 to 512, as said below
- slot_mb: int32 [4, 16], P('dp', 'mb'), may hold values from 0 to 15, each once within a row
Outputs:
- up_grad: float32 [512, 16384], P(('mb', 'dp'), 'tp')
- running_down: float32 [8, 7168, 512], P('mb', 'tp', 'dp')
The draws below stay inside these ranges and needn't reach their ends.
Inputs may be any that keep to these rules, and one draw needn't show every extreme that they name: `mb_tokens`: each count is a multiple of 128; in every group some microbatch has exactly 512 tokens. `slot_mb`: each row is a permutation of the microbatch numbers.
All inputs are finite; a program needn't handle non-finite values.
Results may differ from the reference program's by a relative error of at most 0.005.
Values may be sent and summed in bfloat16 or wider, within the bound.
A program may use at most 128 MiB of HBM per device.

```python
import jax
import jax.numpy as jnp
from jax import lax

D = 7168
R = 512
COLS = 16384
TOKBLOCK = 128
CAP = 512
SLOTS = 2
MICRO = 16
GROUPS = 4
N_MB = 8


def draw_mb_tokens(key, part):
    first_key, second_key = jax.random.split(jax.random.fold_in(key, 11))
    blocks = jax.random.randint(first_key, (GROUPS, MICRO), 1, CAP // TOKBLOCK + 1)
    chosen = jax.random.randint(second_key, (GROUPS, 1), 0, MICRO)
    blocks = jnp.where(jnp.arange(MICRO)[None, :] == chosen, CAP // TOKBLOCK, blocks)
    return (blocks * TOKBLOCK).astype(jnp.int32)


def block_scale(own_key, dims, cuts, smallest, top_value):
    level, own = 1.0, jax.random.fold_in(own_key, 6)
    for axis_at, shards_of in cuts:
        steps = jnp.exp(jax.random.uniform(jax.random.fold_in(own, axis_at), (shards_of,), jnp.float32, smallest / len(cuts), top_value / len(cuts)))
        level = level * jnp.repeat(steps, dims[axis_at] // shards_of).reshape([-1 if axis == axis_at else 1 for axis in range(len(dims))])
    return level


def noise(rng, shape, scale, limit, cuts=(), kind=jnp.bfloat16):
    values = jax.random.normal(rng, shape, jnp.float32) * scale
    if len(cuts) > 0:
        values = block_scale(rng, shape, cuts, -0.22, 0.18) * values
    return jnp.clip(values, min=-limit, max=limit).astype(kind)


def setup_inputs(seed: int = 0) -> dict:
    key_of = jax.random.split(jax.random.key(seed), 7)
    return {
        "hidden": noise(key_of[0], (GROUPS, MICRO, CAP, D), 1.0, 6.0, ((0, 4), (1, 8), (3, 8))),
        "latent": noise(key_of[1], (GROUPS, MICRO, CAP, R), 1.0, 6.0, ((0, 4), (1, 8), (3, 8))),
        "out_grad": noise(key_of[2], (GROUPS, MICRO, CAP, COLS), 0.01, 0.059814453, ((0, 4), (1, 8), (3, 8))),
        "up_weight": noise(key_of[3], (R, COLS), COLS ** -0.5, 0.046875, ((1, 8),)),
        "mb_tokens": draw_mb_tokens(jax.random.fold_in(key_of[6], 71), 0),
        "slot_mb": jax.vmap(lambda own: jax.random.permutation(own, MICRO))(jax.random.split(key_of[5], GROUPS)).reshape((GROUPS, MICRO)).astype(jnp.int32),
    }


def reference(hidden, latent, out_grad, up_weight, mb_tokens, slot_mb):
    counts = jnp.take_along_axis(mb_tokens, slot_mb, axis=1).reshape(-1)
    owners = jnp.tile(jnp.arange(MICRO, dtype=jnp.int32) // SLOTS, GROUPS)
    positions = jnp.arange(CAP, dtype=jnp.int32)

    def accumulate(carry, inputs_now):
        up_total, down_owner = carry
        hidden_rows, latent_rows, grad_rows, length, owner_id = inputs_now
        masked = jnp.where((positions < length)[:, None], grad_rows, jnp.zeros((), grad_rows.dtype))
        latent_grad = jnp.dot(masked, up_weight.T, preferred_element_type=jnp.float32).astype(jnp.bfloat16)
        up_total = up_total + jnp.dot(latent_rows.T, masked, preferred_element_type=jnp.float32)
        down_term = jnp.dot(hidden_rows.T, latent_grad, preferred_element_type=jnp.float32)
        down_owner = down_owner.at[owner_id].add(down_term)
        return (up_total, down_owner), None

    start_state = (jnp.zeros((R, COLS), jnp.float32), jnp.zeros((N_MB, D, R), jnp.float32))
    sequence = (hidden.reshape(-1, CAP, D), latent.reshape(-1, CAP, R), out_grad.reshape(-1, CAP, COLS), counts, owners)
    (up_total, down_owner), unused = lax.scan(accumulate, start_state, sequence)
    return up_total, jnp.cumsum(down_owner, axis=0)
```

```python
import functools

import jax
import jax.numpy as jnp
from jax import lax
from jax.experimental import pallas as pl
from jax.experimental.pallas import tpu as pltpu
from jax.sharding import PartitionSpec as P

MESH = pl.DeviceIdType.MESH
F32 = jnp.float32
BF16 = jnp.bfloat16
NT = (((1,), (1,)), ((), ()))
NN = (((1,), (0,)), ((), ()))
NH = 2
NU = 4


def dot(a, b, dims):
    return lax.dot_general(a, b, dims, preferred_element_type=F32)


class Sems:
    def __init__(self, send, recv):
        self.send, self.recv, self.used = send, recv, 0

    def take(self):
        at = self.used
        self.used += 1
        return self.send.at[at], self.recv.at[at]


def kernel(
    n_z, n_y, n_x,
    hidden, latent, out_grad, weight, tokens, slots,
    up_out, down_out,
    lat_v, h_v, g_v, w_v, lat_all,
    pair_s, pair_r, lg_s, lg_b, lg_far, lg_near, lg_all,
    d_s, d_b, d_far, d_near, zs_d, zr_d, po_d, rf_d,
    u_b, u_far, u_near, zs_u, zr_u,
    load, send, recv,
):
    z = lax.axis_index("mb")
    tp = lax.axis_index("tp")
    x = lax.axis_index("dp")
    y, c = tp // 2, tp % 2
    oc = 1 - c
    cap = g_v.shape[1]
    blk = cap // n_y
    rows_h = lg_all.shape[1]
    rx = rows_h // n_x
    width = h_v.shape[1]
    columns = g_v.shape[2]
    nq = columns // NU

    def tp_of(row, core):
        return lax.rem(row + 2 * n_y, n_y) * 2 + core

    y_up, y_dn, y_far = tp_of(y + 1, c), tp_of(y - 1, c), tp_of(y + 2, c)
    x_up, x_dn, x_far = lax.rem(x + 1, n_x), lax.rem(x + n_x - 1, n_x), lax.rem(x + 2, n_x)
    partner = tp_of(y, oc)
    peers = [{"tp": partner}, {"tp": y_up}, {"tp": y_dn}, {"dp": x_up}, {"dp": x_dn}]
    z_peers = [lax.rem(z + d, n_z) for d in range(1, n_z)]
    peers += [{"mb": p} for p in z_peers]

    loads = []

    def fetch(src, dst):
        copy = pltpu.make_async_copy(src, dst, load.at[len(loads)])
        copy.start()
        loads.append(copy)
        return copy

    barrier = pltpu.get_barrier_semaphore()
    for peer in peers:
        pl.semaphore_signal(barrier, inc=1, device_id=peer, device_id_type=MESH)
    get_lat = fetch(latent, lat_v)
    get_w = [fetch(weight.at[:, 0], w_v.at[0])]
    get_g_other = fetch(out_grad.at[oc], g_v.at[oc])
    get_g_own = fetch(out_grad.at[c], g_v.at[c])
    get_w += [fetch(weight.at[:, h], w_v.at[h]) for h in range(1, NH)]
    get_h = fetch(hidden, h_v)

    sent = []
    sems = Sems(send, recv)

    def ship(src, dst, device, pair):
        copy = pltpu.make_async_remote_copy(
            src_ref=src, dst_ref=dst, send_sem=pair[0], recv_sem=pair[1],
            device_id=device, device_id_type=MESH,
        )
        copy.start()
        sent.append(copy)

    def arrive(dst, pair):
        pltpu.make_async_remote_copy(
            src_ref=dst, dst_ref=dst, send_sem=pair[0], recv_sem=pair[1],
            device_id={"tp": partner}, device_id_type=MESH,
        ).wait_recv()

    count = [tokens[0, slots[0, s]] for s in range(2)]

    get_lat.wait()
    n_lat = lat_v.shape[1]
    eye = (
        lax.broadcasted_iota(jnp.int32, (n_lat, n_lat), 0)
        == lax.broadcasted_iota(jnp.int32, (n_lat, n_lat), 1)
    ).astype(F32).astype(BF16)
    for s in range(2):
        part = dot(eye, lat_v[s * cap : (s + 1) * cap, :], NT)
        position = lax.broadcasted_iota(jnp.int32, part.shape, 1)
        part = jnp.where(position < count[s], part, 0.0).astype(BF16)
        for b in range(n_x):
            lat_all[b, tp, :, s * cap : (s + 1) * cap] = part[b * n_lat // n_x : (b + 1) * n_lat // n_x]
    pl.semaphore_wait(barrier, len(peers))

    def gather(block, half):
        pairs = [sems.take() for _ in range(8)]

        def start():
            ship(block(tp), block(tp), {"tp": y_up}, pairs[0])
            ship(block(tp), block(tp), {"tp": y_dn}, pairs[1])
            ship(block(tp), block(tp), {"tp": partner}, pairs[2])

        def forward():
            arrive(block(y_dn), pairs[0])
            ship(half(y_dn, 0), half(y_dn, 0), {"tp": y_up}, pairs[3])
            ship(block(y_dn), block(y_dn), {"tp": partner}, pairs[5])
            arrive(block(y_up), pairs[1])
            ship(half(y_up, 1), half(y_up, 1), {"tp": y_dn}, pairs[4])
            ship(block(y_up), block(y_up), {"tp": partner}, pairs[6])

        def forward_far():
            arrive(half(y_far, 0), pairs[3])
            arrive(half(y_far, 1), pairs[4])
            ship(block(y_far), block(y_far), {"tp": partner}, pairs[7])

        def finish():
            arrive(block(tp_of(y, oc)), pairs[2])
            arrive(block(tp_of(y - 1, oc)), pairs[5])
            arrive(block(tp_of(y + 1, oc)), pairs[6])
            arrive(block(tp_of(y + 2, oc)), pairs[7])

        return start, forward, forward_far, finish

    def ring_sum(value, block, far, near, size, me, up, dn, across, device):
        pairs = [sems.take() for _ in range(6)]

        def first():
            ship(block(across, 0), far(0), device(up), pairs[0])
            ship(block(across, 1), far(1), device(dn), pairs[1])
            ship(block(up, 1), near(0, 1), device(up), pairs[2])
            ship(block(dn, 0), near(1, 0), device(dn), pairs[3])

        def second():
            arrive(far(0), pairs[0])
            block(up, 0)[...] = (value(up, 0) + far(0)[...].astype(F32)).astype(BF16)
            ship(block(up, 0), near(0, 0), device(up), pairs[4])
            arrive(far(1), pairs[1])
            block(dn, 1)[...] = (value(dn, 1) + far(1)[...].astype(F32)).astype(BF16)
            ship(block(dn, 1), near(1, 1), device(dn), pairs[5])

        def total():
            arrive(near(0, 1), pairs[2])
            arrive(near(1, 0), pairs[3])
            arrive(near(0, 0), pairs[4])
            arrive(near(1, 1), pairs[5])
            return [
                value(me, k) + near(0, k)[...].astype(F32) + near(1, k)[...].astype(F32)
                for k in range(2)
            ]

        return first, second, total

    lat_gather = gather(
        lambda i: lat_all.at[:, i],
        lambda i, k: lat_all.at[pl.ds(k * n_x // 2, n_x // 2), i],
    )

    pair_pairs = [sems.take() for _ in range(NH)]

    def weights(h):
        return w_v[h].reshape(rows_h, columns)

    def other_slot(h):
        pair_s[h] = dot(weights(h), g_v[oc], NT)
        ship(pair_s.at[h], pair_r.at[h], {"tp": partner}, pair_pairs[h])

    def own_slot(h):
        part = dot(weights(h), g_v[c], NT)
        for j in range(n_y):
            lg_s[h, j] = part[:, j * blk : (j + 1) * blk]

    def pair_sum(h):
        arrive(pair_r.at[h], pair_pairs[h])
        for j in range(n_y):
            both = lg_s[h, j] + pair_r[h, :, j * blk : (j + 1) * blk]
            lg_s[h, j] = both
            lg_b[h, j] = both.astype(BF16)

    def row_half(k, rows):
        return pl.ds(k * rows // 2, rows // 2)

    def lg_ring(h):
        return ring_sum(
            lambda j, k: lg_s[h, j, row_half(k, rows_h)],
            lambda j, k: lg_b.at[h, j, row_half(k, rows_h)],
            lambda k: lg_far.at[h, k],
            lambda s, k: lg_near.at[h, s, k],
            rows_h, y, lax.rem(y + 1, n_y), lax.rem(y + n_y - 1, n_y), lax.rem(y + 2, n_y),
            lambda j: {"tp": j * 2 + c},
        )

    lg_rings = [lg_ring(h) for h in range(NH)]

    def lg_gather(h):
        def columns_of(i):
            start = pl.multiple_of(lax.rem(i, 2) * cap + (i // 2) * blk, blk)
            return pl.ds(start, blk)

        return gather(
            lambda i: lg_all.at[h, :, columns_of(i)],
            lambda i, k: lg_all.at[h, row_half(k, rows_h), columns_of(i)],
        )

    lg_gathers = [lg_gather(h) for h in range(NH)]
    live = jnp.where(c == 0, count[0], count[1]) > y * blk

    def lg_final(h):
        for k, part in enumerate(lg_rings[h][2]()):
            start = pl.multiple_of(c * cap + y * blk, blk)
            part = jnp.where(live, part, 0.0).astype(BF16)
            lg_all[h, row_half(k, rows_h), pl.ds(start, blk)] = part
        lg_gathers[h][0]()

    def up_ring(q):
        return ring_sum(
            lambda j, k: u_b[q, j, row_half(k, u_b.shape[2])].astype(F32),
            lambda j, k: u_b.at[q, j, row_half(k, u_b.shape[2])],
            lambda k: u_far.at[q, k],
            lambda s, k: u_near.at[q, s, k],
            u_b.shape[2], x, x_up, x_dn, x_far, lambda j: {"dp": j},
        )

    up_rings = [up_ring(q) for q in range(NU)]

    def up_part(q):
        lhs = lat_all[...].reshape(-1, 2 * cap)
        rhs = g_v[:, :, q * nq : (q + 1) * nq].reshape(2 * cap, nq)
        part = dot(lhs, rhs, NN)
        for b in range(n_x):
            u_b[q, b] = part[b * u_b.shape[2] : (b + 1) * u_b.shape[2]].astype(BF16)
        up_rings[q][0]()

    up_pairs = [[sems.take() for _ in z_peers] for _ in range(NU)]

    def up_scatter(q):
        halves = up_rings[q][2]()
        per_half = n_z // 2
        for k in range(2):
            zs_u[q, k * per_half : (k + 1) * per_half] = (
                halves[k].reshape(per_half, -1, nq).astype(BF16)
            )
        zr_u[q, z] = zs_u[q, z]
        for p, pair in zip(z_peers, up_pairs[q]):
            ship(zs_u.at[q, p], zr_u.at[q, z], {"mb": p}, pair)

    def up_total(q):
        for d, pair in enumerate(up_pairs[q]):
            arrive(zr_u.at[q, lax.rem(z + n_z - 1 - d, n_z)], pair)
        total = zr_u[q, 0].astype(F32)
        for p in range(1, n_z):
            total += zr_u[q, p].astype(F32)
        up_out[:, q * nq : (q + 1) * nq] = total

    def down_ring(h):
        return ring_sum(
            lambda j, k: d_s[h, j, row_half(k, rx)],
            lambda j, k: d_b.at[h, j, row_half(k, rx)],
            lambda k: d_far.at[h, k],
            lambda s, k: d_near.at[h, s, k],
            rx, x, x_up, x_dn, x_far, lambda j: {"dp": j},
        )

    down_rings = [down_ring(h) for h in range(NH)]

    def down_part(h):
        lhs = lg_all[h]
        for start in range(0, width, 256):
            stop = min(start + 256, width)
            part = dot(lhs, h_v[:, start:stop], NN)
            for j in range(n_x):
                rows = part[j * rx : (j + 1) * rx]
                d_s[h, j, :, start:stop] = rows
                d_b[h, j, :, start:stop] = rows.astype(BF16)
        down_rings[h][0]()

    out_pairs = [[sems.take() for _ in z_peers] for _ in range(NH)]
    back_pairs = [[sems.take() for _ in z_peers] for _ in range(NH)]

    def down_scatter(h):
        halves = down_rings[h][2]()
        per_half = n_z // 2
        for k in range(2):
            zs_d[h, k * per_half : (k + 1) * per_half] = (
                halves[k].reshape(per_half, -1, width).astype(BF16)
            )
        zr_d[h, z] = zs_d[h, z]
        for p, pair in zip(z_peers, out_pairs[h]):
            ship(zs_d.at[h, p], zr_d.at[h, z], {"mb": p}, pair)

    def down_prefix(h):
        for d, pair in enumerate(out_pairs[h]):
            arrive(zr_d.at[h, lax.rem(z + n_z - 1 - d, n_z)], pair)
        total = zr_d[h, 0].astype(F32)
        po_d[h, 0] = total.astype(BF16)
        for p in range(1, n_z):
            total += zr_d[h, p].astype(F32)
            po_d[h, p] = total.astype(BF16)
        rf_d[h, z] = po_d[h, z]
        for p, pair in zip(z_peers, back_pairs[h]):
            ship(po_d.at[h, p], rf_d.at[h, z], {"mb": p}, pair)

    def down_arrive(h):
        for d, pair in enumerate(back_pairs[h]):
            arrive(rf_d.at[h, lax.rem(z + n_z - 1 - d, n_z)], pair)

    lat_gather[0]()
    get_w[0].wait()
    get_g_other.wait()
    other_slot(0)
    get_g_own.wait()
    own_slot(0)
    for h in range(1, NH):
        get_w[h].wait()
        other_slot(h)
        pair_sum(h - 1)
        lg_rings[h - 1][0]()
        own_slot(h)
    pair_sum(NH - 1)
    lg_rings[NH - 1][0]()
    lat_gather[1]()
    for h in range(NH):
        lg_rings[h][1]()
    lat_gather[2]()
    lat_gather[3]()
    for h in range(NH):
        up_part(h)
        lg_final(h)
    up_part(2)
    lg_gathers[0][1]()
    up_part(3)
    lg_gathers[1][1]()
    up_rings[0][1]()
    lg_gathers[0][2]()
    lg_gathers[1][2]()
    get_h.wait()
    for h in range(NH):
        lg_gathers[h][3]()
        down_part(h)
    for q in range(1, NU):
        up_rings[q][1]()
    for h in range(NH):
        down_rings[h][1]()
    for q in range(NU):
        up_scatter(q)
    for h in range(NH):
        down_scatter(h)
    for h in range(NH):
        down_prefix(h)
    for q in range(NU):
        up_total(q)
    for h in range(NH):
        down_arrive(h)
    final = rf_d[...].astype(F32).reshape(NH * rx, width)
    down_out[...] = final.T
    for copy in sent:
        copy.wait_send()


def local(sizes, hidden, latent, out_grad, up_weight, mb_tokens, slot_mb):
    n_z, n_y, n_x = sizes
    slot_count, cap, width = hidden.shape[1:]
    rank, columns = up_weight.shape
    n_lat = latent.shape[3]
    row_total = slot_count * cap
    rows_h = rank // NH
    rx = rows_h // n_x
    blk = cap // n_y
    rows_u = rank // n_x
    nq = columns // NU
    any_space = pl.BlockSpec(memory_space=pl.ANY)
    n_sems = 8 + NH + 6 * NH + 8 * NH + 6 * NU + (n_z - 1) * NU + 6 * NH + 2 * (n_z - 1) * NH
    up_grad, running = pl.pallas_call(
        functools.partial(kernel, n_z, n_y, n_x),
        out_shape=(
            jax.ShapeDtypeStruct((rows_u // n_z, columns), F32),
            jax.ShapeDtypeStruct((width, rank // n_x), F32),
        ),
        in_specs=[any_space] * 4 + [pl.BlockSpec(memory_space=pltpu.SMEM)] * 2,
        out_specs=(pl.BlockSpec(memory_space=pltpu.VMEM),) * 2,
        scratch_shapes=[
            pltpu.VMEM((row_total, n_lat), BF16),
            pltpu.VMEM((row_total, width), BF16),
            pltpu.VMEM((slot_count, cap, columns), BF16),
            pltpu.VMEM((NH, n_x, rx, columns), BF16),
            pltpu.VMEM((n_x, 2 * n_y, n_lat // n_x, row_total), BF16),
            pltpu.VMEM((NH, rows_h, cap), F32),
            pltpu.VMEM((NH, rows_h, cap), F32),
            pltpu.VMEM((NH, n_y, rows_h, blk), F32),
            pltpu.VMEM((NH, n_y, rows_h, blk), BF16),
            pltpu.VMEM((NH, 2, rows_h // 2, blk), BF16),
            pltpu.VMEM((NH, 2, 2, rows_h // 2, blk), BF16),
            pltpu.VMEM((NH, rows_h, row_total), BF16),
            pltpu.VMEM((NH, n_x, rx, width), F32),
            pltpu.VMEM((NH, n_x, rx, width), BF16),
            pltpu.VMEM((NH, 2, rx // 2, width), BF16),
            pltpu.VMEM((NH, 2, 2, rx // 2, width), BF16),
            pltpu.VMEM((NH, n_z, rx // n_z, width), BF16),
            pltpu.VMEM((NH, n_z, rx // n_z, width), BF16),
            pltpu.VMEM((NH, n_z, rx // n_z, width), BF16),
            pltpu.VMEM((NH, n_z, rx // n_z, width), BF16),
            pltpu.VMEM((NU, n_x, rows_u, nq), BF16),
            pltpu.VMEM((NU, 2, rows_u // 2, nq), BF16),
            pltpu.VMEM((NU, 2, 2, rows_u // 2, nq), BF16),
            pltpu.VMEM((NU, n_z, rows_u // n_z, nq), BF16),
            pltpu.VMEM((NU, n_z, rows_u // n_z, nq), BF16),
            pltpu.SemaphoreType.DMA((8,)),
            pltpu.SemaphoreType.DMA((n_sems,)),
            pltpu.SemaphoreType.DMA((n_sems,)),
        ],
        compiler_params=pltpu.CompilerParams(
            collective_id=0, has_side_effects=True, vmem_limit_bytes=62 * 1024 * 1024
        ),
    )(
        hidden.reshape(row_total, width),
        latent.reshape(row_total, n_lat),
        out_grad.reshape(slot_count, cap, columns),
        up_weight.reshape(n_x, NH, rx, columns),
        mb_tokens,
        slot_mb,
    )
    return up_grad, running[None]


def solution(mesh):
    sizes = (mesh.shape["mb"], mesh.shape["tp"] // 2, mesh.shape["dp"])
    return jax.shard_map(
        functools.partial(local, sizes),
        mesh=mesh,
        in_specs=(
            P("dp", "mb", None, "tp"),
            P("dp", "mb", None, "tp"),
            P("dp", "mb", None, "tp"),
            P(None, "tp"),
            P("dp", None),
            P("dp", "mb"),
        ),
        out_specs=(P(("mb", "dp"), "tp"), P("mb", "tp", "dp")),
        check_vma=False,
    )
```

```python
import collections
import functools

import jax
import jax.numpy as jnp
from jax import lax
from jax.experimental import pallas as pl
from jax.experimental.pallas import tpu as pltpu
from jax.sharding import PartitionSpec as P

MESH = pl.DeviceIdType.MESH
F32 = jnp.float32
BF16 = jnp.bfloat16
NT = (((1,), (1,)), ((), ()))
NN = (((1,), (0,)), ((), ()))
NH = 2
NG = 4


def dot(a, b, dims):
    return lax.dot_general(a, b, dims, preferred_element_type=F32)


Gather = collections.namedtuple(
    "Gather", ["near", "across", "along", "across_halves", "far", "across_far", "finish"]
)
Ring = collections.namedtuple("Ring", ["far", "near", "second", "total"])


class Sems:
    def __init__(self, send, recv):
        self.send, self.recv, self.used = send, recv, 0

    def take(self):
        at = self.used
        self.used += 1
        return self.send.at[at], self.recv.at[at]


def kernel(
    n_z, n_y, n_x,
    hidden, latent, out_grad, weight, tokens_in, slots_in,
    up_out, down_out,
    tokens, slots,
    lat_v, h_v, g_v, w_v, lat_all,
    pair_s, pair_r, lg_s, lg_b, lg_in, lg_all,
    d_s, d_b, d_far, d_near, zs_d, zr_d, po_d, rf_d,
    u_b, u_far, u_near, t_u, t_pair, f_u, zr_u,
    load, send, recv,
):
    z = lax.axis_index("mb")
    tp = lax.axis_index("tp")
    x = lax.axis_index("dp")
    y, c = tp // 2, tp % 2
    oc = 1 - c
    cap = g_v.shape[1]
    blk = cap // n_y
    rows_h = lg_all.shape[1]
    rx = rows_h // n_x
    width = h_v.shape[1]
    columns = g_v.shape[2]
    half_c = columns // 2
    split = (width // 2 + 127) // 128 * 128

    def tp_of(row, core):
        return lax.rem(row + 2 * n_y, n_y) * 2 + core

    y_up, y_dn, y_far = tp_of(y + 1, c), tp_of(y - 1, c), tp_of(y + 2, c)
    x_up, x_dn, x_far = lax.rem(x + 1, n_x), lax.rem(x + n_x - 1, n_x), lax.rem(x + 2, n_x)
    partner = tp_of(y, oc)
    peers = [{"tp": partner}, {"tp": y_up}, {"tp": y_dn}]
    peers += [{"tp": y_far}]
    peers += [{"dp": x_up}, {"dp": x_dn}]
    hops = sorted(range(1, n_z), key=lambda d: -min(d, n_z - d))
    z_peers = [lax.rem(z + d, n_z) for d in hops]
    z_sources = [lax.rem(z + n_z - d, n_z) for d in hops]
    peers += [{"mb": p} for p in z_peers]

    loads = []

    def fetch(src, dst):
        copy = pltpu.make_async_copy(src, dst, load.at[len(loads)])
        copy.start()
        loads.append(copy)
        return copy

    barrier = pltpu.get_barrier_semaphore()
    for peer in peers:
        pl.semaphore_signal(barrier, inc=1, device_id=peer, device_id_type=MESH)
    get_lat = fetch(latent, lat_v)
    get_scalars = [fetch(tokens_in, tokens), fetch(slots_in, slots)]
    get_w = [fetch(weight.at[:, 0], w_v.at[0])]
    get_g_other = fetch(out_grad.at[oc], g_v.at[oc])
    get_g_own = fetch(out_grad.at[c], g_v.at[c])
    get_w += [fetch(weight.at[:, h], w_v.at[h]) for h in range(1, NH)]
    get_h = fetch(hidden, h_v)

    sent = []
    sems = Sems(send, recv)

    def ship(src, dst, device, pair):
        copy = pltpu.make_async_remote_copy(
            src_ref=src, dst_ref=dst, send_sem=pair[0], recv_sem=pair[1],
            device_id=device, device_id_type=MESH,
        )
        copy.start()
        sent.append(copy)

    def arrive(dst, pair):
        pltpu.make_async_remote_copy(
            src_ref=dst, dst_ref=dst, send_sem=pair[0], recv_sem=pair[1],
            device_id={"tp": partner}, device_id_type=MESH,
        ).wait_recv()

    for copy in get_scalars:
        copy.wait()
    count = [tokens[0, slots[0, s]] for s in range(2)]

    get_lat.wait()
    n_lat = lat_v.shape[1]
    for s in range(2):
        part = lat_v[s].astype(F32)
        position = lax.broadcasted_iota(jnp.int32, part.shape, 1)
        part = jnp.where(position < count[s], part, 0.0).astype(BF16)
        lat_all[tp, :, s * cap : (s + 1) * cap] = part
    pl.semaphore_wait(barrier, len(peers))

    def row_half(k, rows):
        return pl.ds(k * rows // 2, rows // 2)

    def gather(block, half):
        pairs = [sems.take() for _ in range(8)]

        def near():
            ship(block(tp), block(tp), {"tp": y_up}, pairs[0])
            ship(block(tp), block(tp), {"tp": y_dn}, pairs[1])
            ship(block(tp), block(tp), {"tp": partner}, pairs[2])

        def across():
            arrive(block(y_dn), pairs[0])
            ship(block(y_dn), block(y_dn), {"tp": partner}, pairs[5])
            arrive(block(y_up), pairs[1])
            ship(block(y_up), block(y_up), {"tp": partner}, pairs[6])

        def along():
            ship(half(y_dn, 0), half(y_dn, 0), {"tp": y_up}, pairs[3])
            ship(half(y_up, 1), half(y_up, 1), {"tp": y_dn}, pairs[4])

        def across_halves():
            arrive(half(y_far, 0), pairs[3])
            arrive(half(y_far, 1), pairs[4])
            ship(block(y_far), block(y_far), {"tp": partner}, pairs[7])

        def far():
            ship(block(tp), block(tp), {"tp": y_far}, pairs[3])

        def across_far():
            arrive(block(y_far), pairs[3])
            ship(block(y_far), block(y_far), {"tp": partner}, pairs[7])

        def finish(*which):
            for k in which:
                arrive(block(tp_of(y + (0, -1, 1, 2)[k], oc)), pairs[(2, 5, 6, 7)[k]])

        return Gather(near, across, along, across_halves, far, across_far, finish)

    def ring_sum(value, block, far, near, me, up, dn, across, device):
        pairs = [sems.take() for _ in range(6)]

        def send_far():
            ship(block(across, 0), far(0), device(up), pairs[0])
            ship(block(across, 1), far(1), device(dn), pairs[1])

        def send_near():
            ship(block(up, 1), near(0, 1), device(up), pairs[2])
            ship(block(dn, 0), near(1, 0), device(dn), pairs[3])

        def second():
            arrive(far(0), pairs[0])
            block(up, 0)[...] = (value(up, 0) + far(0)[...].astype(F32)).astype(BF16)
            ship(block(up, 0), near(0, 0), device(up), pairs[4])
            arrive(far(1), pairs[1])
            block(dn, 1)[...] = (value(dn, 1) + far(1)[...].astype(F32)).astype(BF16)
            ship(block(dn, 1), near(1, 1), device(dn), pairs[5])

        def total():
            arrive(near(0, 1), pairs[2])
            arrive(near(1, 0), pairs[3])
            arrive(near(0, 0), pairs[4])
            arrive(near(1, 1), pairs[5])
            return [
                value(me, k) + near(0, k)[...].astype(F32) + near(1, k)[...].astype(F32)
                for k in range(2)
            ]

        return Ring(send_far, send_near, second, total)

    lat_gather = gather(
        lambda i: lat_all.at[i],
        lambda i, k: lat_all.at[i, row_half(k, n_lat)],
    )

    pair_pairs = [sems.take() for _ in range(NH)]

    def weights(h):
        return w_v[h].reshape(rows_h, columns)

    def other_slot(h):
        pair_s[h] = dot(weights(h), g_v[oc], NT)
        ship(pair_s.at[h], pair_r.at[h], {"tp": partner}, pair_pairs[h])

    def own_slot(h):
        part = dot(weights(h), g_v[c], NT)
        for j in range(n_y):
            lg_s[h, j] = part[:, j * blk : (j + 1) * blk]

    def pair_sum(h):
        arrive(pair_r.at[h], pair_pairs[h])
        for j in range(n_y):
            both = lg_s[h, j] + pair_r[h, :, j * blk : (j + 1) * blk]
            lg_s[h, j] = both
            lg_b[h, j] = both.astype(BF16)

    lg_hops = (2, 1, n_y - 1)
    lg_pairs = [[sems.take() for _ in lg_hops] for _ in range(NH)]

    def lg_spread(h):
        for k, hop in enumerate(lg_hops):
            row = lax.rem(y + hop, n_y)
            ship(lg_b.at[h, row], lg_in.at[h, k], {"tp": row * 2 + c}, lg_pairs[h][k])

    def lg_gather(h):
        def columns_of(i):
            start = pl.multiple_of(lax.rem(i, 2) * cap + (i // 2) * blk, blk)
            return pl.ds(start, blk)

        return gather(
            lambda i: lg_all.at[h, :, columns_of(i)],
            lambda i, k: lg_all.at[h, row_half(k, rows_h), columns_of(i)],
        )

    lg_gathers = [lg_gather(h) for h in range(NH)]
    live = jnp.where(c == 0, count[0], count[1]) > y * blk

    def lg_final(h):
        total = lg_s[h, y]
        for k in range(len(lg_hops)):
            arrive(lg_in.at[h, k], lg_pairs[h][k])
            total += lg_in[h, k].astype(F32)
        start = pl.multiple_of(c * cap + y * blk, blk)
        lg_all[h, :, pl.ds(start, blk)] = jnp.where(live, total, 0.0).astype(BF16)
        lg_gathers[h].far()
        lg_gathers[h].near()

    rows_of = [lax.rem(y + n_y + off, n_y) for off in (0, 1, -1, 2)]
    parity = lax.rem(z, 2)
    across_z = [lax.rem(z + n_z + 1 - 2 * lax.rem(z + k, 2), n_z) for k in range(2)]
    swap_pairs = [[sems.take() for _ in range(2)] for _ in range(NG)]

    def column_half(k):
        return pl.ds(k * half_c, half_c)

    def up_ring(g):
        return ring_sum(
            lambda j, k: u_b[g, j, :, :, column_half(k)].astype(F32),
            lambda j, k: u_b.at[g, j, :, :, column_half(k)],
            lambda k: u_far.at[g, k],
            lambda s, k: u_near.at[g, s, k],
            x, x_up, x_dn, x_far, lambda j: {"dp": j},
        )

    up_rings = [up_ring(g) for g in range(NG)]

    def up_part(g):
        rows = n_lat // n_x
        lhs = lat_all[pl.ds(rows_of[g] * 2, 2)].reshape(2 * n_lat, 2 * cap)
        step = 512
        for start in range(0, columns, step):
            rhs = g_v[:, :, start : start + step].reshape(2 * cap, step)
            part = dot(lhs, rhs, NN).astype(BF16)
            for k in range(2):
                for b in range(n_x):
                    at = k * n_lat + b * rows
                    u_b[g, b, k, :, start : start + step] = part[at : at + rows]

    def up_total(g):
        for k, part in enumerate(up_rings[g].total()):
            t_u[g, :, :, column_half(k)] = part.astype(BF16)
        for k in range(2):
            ship(
                t_u.at[g, 1 - parity, :, column_half(k)], t_pair.at[g, k],
                {"mb": across_z[k]}, swap_pairs[g][k],
            )

    up_hops = range(2, n_z, 2)
    up_base = sems.used
    up_pairs = [sems.take() for _ in up_hops]
    to_owner = []

    def up_owner(g):
        for k in range(2):
            arrive(t_pair.at[g, k], swap_pairs[g][k])
            both = t_u[g, parity, :, column_half(k)].astype(F32) + t_pair[g, k].astype(F32)
            f_u[rows_of[g], :, column_half(k)] = both.astype(BF16)
        owner = 2 * rows_of[g] + parity
        hop = lax.rem(owner - z + n_z, n_z) // 2
        at = lax.rem(hop + n_z // 2 - 1, n_z // 2)
        slot = jnp.minimum(at, n_z // 2 - 2)
        copy = pltpu.make_async_remote_copy(
            src_ref=f_u.at[rows_of[g]], dst_ref=zr_u.at[slot],
            send_sem=send.at[up_base + slot], recv_sem=recv.at[up_base + slot],
            device_id={"mb": owner}, device_id_type=MESH,
        )
        pl.when(owner != z)(copy.start)
        to_owner.append((owner, copy))

    def up_final():
        total = f_u[z // 2].astype(F32)
        for d, pair in enumerate(up_pairs):
            arrive(zr_u.at[d], pair)
            total += zr_u[d].astype(F32)
        up_out[...] = total

    cuts = [(h, lo, hi) for h in range(NH) for lo, hi in ((0, split), (split, width))]

    def down_ring(h, lo, hi):
        return ring_sum(
            lambda j, k: d_s[h, j, row_half(k, rx), lo:hi],
            lambda j, k: d_b.at[h, j, row_half(k, rx), lo:hi],
            lambda k: d_far.at[h, k, :, lo:hi],
            lambda s, k: d_near.at[h, s, k, :, lo:hi],
            x, x_up, x_dn, x_far, lambda j: {"dp": j},
        )

    down_rings = [down_ring(*cut) for cut in cuts]

    def down_part(i):
        h, lo, hi = cuts[i]
        lhs = lg_all[h]
        for start in range(lo, hi, 256):
            stop = min(start + 256, hi)
            part = dot(lhs, h_v[:, start:stop], NN)
            for j in range(n_x):
                rows = part[j * rx : (j + 1) * rx]
                d_s[h, j, :, start:stop] = rows
                d_b[h, j, :, start:stop] = rows.astype(BF16)

    out_pairs = [[sems.take() for _ in z_peers] for _ in cuts]
    back_pairs = [[sems.take() for _ in z_peers] for _ in cuts]

    def down_scatter(i):
        h, lo, hi = cuts[i]
        halves = down_rings[i].total()
        per_half = n_z // 2
        for k in range(2):
            zs_d[h, k * per_half : (k + 1) * per_half, :, lo:hi] = (
                halves[k].reshape(per_half, -1, hi - lo).astype(BF16)
            )
        zr_d[h, z, :, lo:hi] = zs_d[h, z, :, lo:hi]
        for p, pair in zip(z_peers, out_pairs[i]):
            ship(zs_d.at[h, p, :, lo:hi], zr_d.at[h, z, :, lo:hi], {"mb": p}, pair)

    def down_prefix(i):
        h, lo, hi = cuts[i]
        for p, pair in zip(z_sources, out_pairs[i]):
            arrive(zr_d.at[h, p, :, lo:hi], pair)
        total = zr_d[h, 0, :, lo:hi].astype(F32)
        po_d[h, 0, :, lo:hi] = total.astype(BF16)
        for p in range(1, n_z):
            total += zr_d[h, p, :, lo:hi].astype(F32)
            po_d[h, p, :, lo:hi] = total.astype(BF16)
        rf_d[h, z, :, lo:hi] = po_d[h, z, :, lo:hi]
        for p, pair in zip(z_peers, back_pairs[i]):
            ship(po_d.at[h, p, :, lo:hi], rf_d.at[h, z, :, lo:hi], {"mb": p}, pair)

    def down_arrive(i):
        h, lo, hi = cuts[i]
        for p, pair in zip(z_sources, back_pairs[i]):
            arrive(rf_d.at[h, p, :, lo:hi], pair)

    lat_gather.near()
    get_w[0].wait()
    get_g_other.wait()
    other_slot(0)
    get_g_own.wait()
    own_slot(0)
    get_w[1].wait()
    other_slot(1)
    pair_sum(0)
    lg_spread(0)
    own_slot(1)
    pair_sum(1)
    lg_spread(1)
    lat_gather.finish(0)
    up_part(0)
    up_rings[0].far()
    up_rings[0].near()
    lat_gather.across()
    lat_gather.finish(2)
    up_part(1)
    up_rings[1].far()
    lat_gather.finish(1)
    up_part(2)
    up_rings[0].second()
    up_rings[1].near()
    lg_final(0)
    up_rings[2].far()
    lg_final(1)
    lat_gather.along()
    up_rings[1].second()
    up_rings[2].near()
    up_total(0)
    lg_gathers[0].across_far()
    lg_gathers[0].across()
    up_rings[2].second()
    get_h.wait()
    lg_gathers[0].finish(0, 1, 2, 3)
    down_part(0)
    down_rings[0].far()
    down_part(1)
    down_rings[1].far()
    down_rings[0].near()
    down_rings[1].near()
    lg_gathers[1].across_far()
    up_total(1)
    lg_gathers[1].across()
    lg_gathers[1].finish(0, 1, 2, 3)
    down_part(2)
    down_rings[2].far()
    down_part(3)
    down_rings[3].far()
    up_total(2)
    lat_gather.across_halves()
    down_rings[0].second()
    down_rings[1].second()
    down_rings[2].near()
    down_rings[3].near()
    up_owner(0)
    up_owner(1)
    lat_gather.finish(3)
    up_part(3)
    up_owner(2)
    down_rings[2].second()
    down_rings[3].second()
    up_rings[3].far()
    up_rings[3].near()
    down_scatter(0)
    down_scatter(1)
    down_scatter(2)
    down_scatter(3)
    up_rings[3].second()
    down_prefix(0)
    down_prefix(1)
    up_total(3)
    down_prefix(2)
    down_prefix(3)
    up_owner(3)
    down_arrive(0)
    down_arrive(1)
    down_arrive(2)
    down_arrive(3)
    up_final()
    down_out[...] = rf_d[...].astype(F32).reshape(NH * rx, width).astype(BF16)
    for copy in sent:
        copy.wait_send()
    for owner, copy in to_owner:
        pl.when(owner != z)(copy.wait_send)


def finish_kernel(up_in, down_in, up_out, down_out):
    up_out[...] = up_in[...]
    down_out[...] = down_in[...].astype(F32).T


def local(sizes, hidden, latent, out_grad, up_weight, mb_tokens, slot_mb):
    n_z, n_y, n_x = sizes
    slot_count, cap, width = hidden.shape[1:]
    rank, columns = up_weight.shape
    n_lat = latent.shape[3]
    row_total = slot_count * cap
    rows_h = rank // NH
    rx = rows_h // n_x
    blk = cap // n_y
    rows_u = rank // n_x // n_z
    in_hbm = pl.BlockSpec(memory_space=pltpu.HBM)
    n_sems = 8 + NH + 3 * NH + 8 * NH + 8 * NG + (n_z // 2 - 1) + 2 * (6 + 2 * (n_z - 1)) * NH
    up_grad, running = pl.pallas_call(
        functools.partial(kernel, n_z, n_y, n_x),
        out_shape=(
            jax.ShapeDtypeStruct((rows_u, columns), F32),
            jax.ShapeDtypeStruct((rank // n_x, width), BF16),
        ),
        in_specs=[in_hbm] * 6,
        out_specs=(pl.BlockSpec(memory_space=pltpu.VMEM),) * 2,
        scratch_shapes=[
            pltpu.SMEM(mb_tokens.shape, jnp.int32),
            pltpu.SMEM(slot_mb.shape, jnp.int32),
            pltpu.VMEM((slot_count, n_lat, cap), BF16),
            pltpu.VMEM((row_total, width), BF16),
            pltpu.VMEM((slot_count, cap, columns), BF16),
            pltpu.VMEM((NH, n_x, rx, columns), BF16),
            pltpu.VMEM((2 * n_y, n_lat, row_total), BF16),
            pltpu.VMEM((NH, rows_h, cap), F32),
            pltpu.VMEM((NH, rows_h, cap), F32),
            pltpu.VMEM((NH, n_y, rows_h, blk), F32),
            pltpu.VMEM((NH, n_y, rows_h, blk), BF16),
            pltpu.VMEM((NH, 3, rows_h, blk), BF16),
            pltpu.VMEM((NH, rows_h, row_total), BF16),
            pltpu.VMEM((NH, n_x, rx, width), F32),
            pltpu.VMEM((NH, n_x, rx, width), BF16),
            pltpu.VMEM((NH, 2, rx // 2, width), BF16),
            pltpu.VMEM((NH, 2, 2, rx // 2, width), BF16),
            pltpu.VMEM((NH, n_z, rx // n_z, width), BF16),
            pltpu.VMEM((NH, n_z, rx // n_z, width), BF16),
            pltpu.VMEM((NH, n_z, rx // n_z, width), BF16),
            pltpu.VMEM((NH, n_z, rx // n_z, width), BF16),
            pltpu.VMEM((NG, n_x, 2, rows_u, columns), BF16),
            pltpu.VMEM((NG, 2, 2, rows_u, columns // 2), BF16),
            pltpu.VMEM((NG, 2, 2, 2, rows_u, columns // 2), BF16),
            pltpu.VMEM((NG, 2, rows_u, columns), BF16),
            pltpu.VMEM((NG, 2, rows_u, columns // 2), BF16),
            pltpu.VMEM((n_y, rows_u, columns), BF16),
            pltpu.VMEM((n_z // 2 - 1, rows_u, columns), BF16),
            pltpu.SemaphoreType.DMA((10,)),
            pltpu.SemaphoreType.DMA((n_sems,)),
            pltpu.SemaphoreType.DMA((n_sems,)),
        ],
        compiler_params=pltpu.CompilerParams(
            collective_id=0, has_side_effects=True, vmem_limit_bytes=66_400_000
        ),
    )(
        hidden.reshape(row_total, width),
        latent[0].swapaxes(1, 2),
        out_grad.reshape(slot_count, cap, columns),
        up_weight.reshape(n_x, NH, rx, columns),
        mb_tokens,
        slot_mb,
    )
    up_grad, running = pl.pallas_call(
        finish_kernel,
        out_shape=(
            jax.ShapeDtypeStruct((rows_u, columns), F32),
            jax.ShapeDtypeStruct((width, rank // n_x), F32),
        ),
        in_specs=[pl.BlockSpec(memory_space=pltpu.VMEM)] * 2,
        out_specs=(pl.BlockSpec(memory_space=pltpu.VMEM),) * 2,
        compiler_params=pltpu.CompilerParams(vmem_limit_bytes=8 * 1024 * 1024),
    )(up_grad, running)
    return up_grad, running[None]


def solution(mesh):
    sizes = (mesh.shape["mb"], mesh.shape["tp"] // 2, mesh.shape["dp"])
    return jax.shard_map(
        functools.partial(local, sizes),
        mesh=mesh,
        in_specs=(
            P("dp", "mb", None, "tp"),
            P("dp", "mb", None, "tp"),
            P("dp", "mb", None, "tp"),
            P(None, "tp"),
            P("dp", None),
            P("dp", "mb"),
        ),
        out_specs=(P(("mb", "dp"), "tp"), P("mb", "tp", "dp")),
        check_vma=False,
    )
```

```python
import collections
import functools

import jax
import jax.numpy as jnp
from jax import lax
from jax.experimental import pallas as pl
from jax.experimental.pallas import tpu as pltpu
from jax.sharding import PartitionSpec as P

MESH = pl.DeviceIdType.MESH
F32 = jnp.float32
BF16 = jnp.bfloat16
NT = (((1,), (1,)), ((), ()))
NN = (((1,), (0,)), ((), ()))
NH = 2
SWAPPED = 2
NG = 4


def dot(a, b, dims):
    return lax.dot_general(a, b, dims, preferred_element_type=F32)


Gather = collections.namedtuple(
    "Gather", ["near", "across", "along", "across_halves", "far", "across_far", "finish"]
)
Ring = collections.namedtuple("Ring", ["far", "near", "second", "total"])


class Sems:
    def __init__(self, send, recv):
        self.send, self.recv, self.used = send, recv, 0

    def take(self):
        at = self.used
        self.used += 1
        return self.send.at[at], self.recv.at[at]


def kernel(
    n_z, n_y, n_x,
    hidden, latent, out_grad, weight, tokens_in, slots_in,
    zr_u, rf_d,
    tokens, slots,
    lat_v, h_v, g_v, w_v, lat_all,
    pair_s, pair_r, lg_s, lg_b, lg_in, lg_all,
    d_s, d_b, d_far, d_near, zs_d, zr_d, po_d,
    u_b, u_pair, x_b, u_far, u_near, t_u, t_pair, f_u,
    load, save, send, recv,
):
    z = lax.axis_index("mb")
    tp = lax.axis_index("tp")
    x = lax.axis_index("dp")
    y, c = tp // 2, tp % 2
    oc = 1 - c
    cap = g_v.shape[1]
    blk = cap // n_y
    rows_h = lg_all.shape[1]
    rx = rows_h // n_x
    width = h_v.shape[1]
    columns = g_v.shape[2]
    half_c = columns // 2
    split = (width // 2 + 127) // 128 * 128

    def tp_of(row, core):
        return lax.rem(row + 2 * n_y, n_y) * 2 + core

    y_up, y_dn, y_far = tp_of(y + 1, c), tp_of(y - 1, c), tp_of(y + 2, c)
    x_up, x_dn, x_far = lax.rem(x + 1, n_x), lax.rem(x + n_x - 1, n_x), lax.rem(x + 2, n_x)
    partner = tp_of(y, oc)
    peers = [{"tp": partner}, {"tp": y_up}, {"tp": y_dn}]
    peers += [{"tp": y_far}]
    peers += [{"dp": x_up}, {"dp": x_dn}]
    hops = sorted(range(1, n_z), key=lambda d: -min(d, n_z - d))
    z_peers = [lax.rem(z + d, n_z) for d in hops]
    z_sources = [lax.rem(z + n_z - d, n_z) for d in hops]
    peers += [{"mb": p} for p in z_peers]

    loads = []

    def fetch(src, dst):
        copy = pltpu.make_async_copy(src, dst, load.at[len(loads)])
        copy.start()
        loads.append(copy)
        return copy

    barrier = pltpu.get_barrier_semaphore()
    for peer in peers:
        pl.semaphore_signal(barrier, inc=1, device_id=peer, device_id_type=MESH)
    get_lat = fetch(latent, lat_v)
    get_scalars = [fetch(tokens_in, tokens), fetch(slots_in, slots)]
    get_w = [fetch(weight.at[:, 0], w_v.at[0])]
    get_g_other = fetch(out_grad.at[oc], g_v.at[oc])
    get_g_own = fetch(out_grad.at[c], g_v.at[c])
    get_w += [fetch(weight.at[:, h], w_v.at[h]) for h in range(1, NH)]
    get_h = fetch(hidden, h_v)

    sent = []
    kept = []
    sems = Sems(send, recv)

    def keep(src, dst):
        copy = pltpu.make_async_copy(src, dst, save.at[len(kept)])
        copy.start()
        kept.append(copy)

    def ship(src, dst, device, pair):
        copy = pltpu.make_async_remote_copy(
            src_ref=src, dst_ref=dst, send_sem=pair[0], recv_sem=pair[1],
            device_id=device, device_id_type=MESH,
        )
        copy.start()
        sent.append(copy)

    def arrive(dst, pair):
        pltpu.make_async_remote_copy(
            src_ref=dst, dst_ref=dst, send_sem=pair[0], recv_sem=pair[1],
            device_id={"tp": partner}, device_id_type=MESH,
        ).wait_recv()

    for copy in get_scalars:
        copy.wait()
    count = [tokens[0, slots[0, s]] for s in range(2)]

    get_lat.wait()
    n_lat = lat_v.shape[1]
    for s in range(2):
        part = lat_v[s].astype(F32)
        position = lax.broadcasted_iota(jnp.int32, part.shape, 1)
        part = jnp.where(position < count[s], part, 0.0).astype(BF16)
        lat_all[tp, :, s * cap : (s + 1) * cap] = part
    pl.semaphore_wait(barrier, len(peers))

    def row_half(k, rows):
        return pl.ds(k * rows // 2, rows // 2)

    def gather(block, half):
        pairs = [sems.take() for _ in range(8)]

        def near():
            ship(block(tp), block(tp), {"tp": y_up}, pairs[0])
            ship(block(tp), block(tp), {"tp": y_dn}, pairs[1])
            ship(block(tp), block(tp), {"tp": partner}, pairs[2])

        def across():
            arrive(block(y_dn), pairs[0])
            ship(block(y_dn), block(y_dn), {"tp": partner}, pairs[5])
            arrive(block(y_up), pairs[1])
            ship(block(y_up), block(y_up), {"tp": partner}, pairs[6])

        def along():
            ship(half(y_dn, 0), half(y_dn, 0), {"tp": y_up}, pairs[3])
            ship(half(y_up, 1), half(y_up, 1), {"tp": y_dn}, pairs[4])

        def across_halves():
            arrive(half(y_far, 0), pairs[3])
            arrive(half(y_far, 1), pairs[4])
            ship(block(y_far), block(y_far), {"tp": partner}, pairs[7])

        def far():
            ship(block(tp), block(tp), {"tp": y_far}, pairs[3])

        def across_far():
            arrive(block(y_far), pairs[3])
            ship(block(y_far), block(y_far), {"tp": partner}, pairs[7])

        def finish(*which):
            for k in which:
                arrive(block(tp_of(y + (0, -1, 1, 2)[k], oc)), pairs[(2, 5, 6, 7)[k]])

        return Gather(near, across, along, across_halves, far, across_far, finish)

    def ring_sum(value, block, far, near, me, up, dn, across, device):
        pairs = [sems.take() for _ in range(6)]

        def send_far():
            ship(block(across, 0), far(0), device(up), pairs[0])
            ship(block(across, 1), far(1), device(dn), pairs[1])

        def send_near():
            ship(block(up, 1), near(0, 1), device(up), pairs[2])
            ship(block(dn, 0), near(1, 0), device(dn), pairs[3])

        def second():
            arrive(far(0), pairs[0])
            block(up, 0)[...] = (value(up, 0) + far(0)[...].astype(F32)).astype(BF16)
            ship(block(up, 0), near(0, 0), device(up), pairs[4])
            arrive(far(1), pairs[1])
            block(dn, 1)[...] = (value(dn, 1) + far(1)[...].astype(F32)).astype(BF16)
            ship(block(dn, 1), near(1, 1), device(dn), pairs[5])

        def total():
            arrive(near(0, 1), pairs[2])
            arrive(near(1, 0), pairs[3])
            arrive(near(0, 0), pairs[4])
            arrive(near(1, 1), pairs[5])
            return [
                value(me, k) + near(0, k)[...].astype(F32) + near(1, k)[...].astype(F32)
                for k in range(2)
            ]

        return Ring(send_far, send_near, second, total)

    lat_gather = gather(
        lambda i: lat_all.at[i],
        lambda i, k: lat_all.at[i, row_half(k, n_lat)],
    )

    pair_pairs = [sems.take() for _ in range(NH)]

    def weights(h):
        return w_v[h].reshape(rows_h, columns)

    def other_slot(h):
        pair_s[h] = dot(weights(h), g_v[oc], NT)
        ship(pair_s.at[h], pair_r.at[h], {"tp": partner}, pair_pairs[h])

    def own_slot(h):
        part = dot(weights(h), g_v[c], NT)
        for j in range(n_y):
            lg_s[h, j] = part[:, j * blk : (j + 1) * blk]

    def pair_sum(h):
        arrive(pair_r.at[h], pair_pairs[h])
        for j in range(n_y):
            both = lg_s[h, j] + pair_r[h, :, j * blk : (j + 1) * blk]
            lg_s[h, j] = both
            lg_b[h, j] = both.astype(BF16)

    lg_hops = (2, 1, n_y - 1)
    lg_pairs = [[sems.take() for _ in lg_hops] for _ in range(NH)]

    def lg_spread(h):
        for k, hop in enumerate(lg_hops):
            row = lax.rem(y + hop, n_y)
            ship(lg_b.at[h, row], lg_in.at[h, k], {"tp": row * 2 + c}, lg_pairs[h][k])

    def lg_gather(h):
        def columns_of(i):
            start = pl.multiple_of(lax.rem(i, 2) * cap + (i // 2) * blk, blk)
            return pl.ds(start, blk)

        return gather(
            lambda i: lg_all.at[h, :, columns_of(i)],
            lambda i, k: lg_all.at[h, row_half(k, rows_h), columns_of(i)],
        )

    lg_gathers = [lg_gather(h) for h in range(NH)]
    live = jnp.where(c == 0, count[0], count[1]) > y * blk

    def lg_final(h):
        total = lg_s[h, y]
        for k in range(len(lg_hops)):
            arrive(lg_in.at[h, k], lg_pairs[h][k])
            total += lg_in[h, k].astype(F32)
        start = pl.multiple_of(c * cap + y * blk, blk)
        lg_all[h, :, pl.ds(start, blk)] = jnp.where(live, total, 0.0).astype(BF16)
        lg_gathers[h].far()
        lg_gathers[h].near()

    rows_of = [lax.rem(y + n_y + off, n_y) for off in (0, 1, -1, 2)]
    parity = lax.rem(z, 2)
    across_z = [lax.rem(z + n_z + 1 - 2 * lax.rem(z + k, 2), n_z) for k in range(2)]
    swap_pairs = [[sems.take() for _ in range(2)] for _ in range(NG)]

    def column_half(k):
        return pl.ds(k * half_c, half_c)

    def up_ring(g):
        if g == SWAPPED:
            return ring_sum(
                lambda j, k: x_b[j, :, column_half(k)].astype(F32),
                lambda j, k: x_b.at[j, :, column_half(k)],
                lambda k: u_far.at[g, k, 0],
                lambda s, k: u_near.at[g, s, k, 0],
                x, x_up, x_dn, x_far, lambda j: {"dp": j},
            )
        return ring_sum(
            lambda j, k: u_b[g, j, :, :, column_half(k)].astype(F32),
            lambda j, k: u_b.at[g, j, :, :, column_half(k)],
            lambda k: u_far.at[g, k],
            lambda s, k: u_near.at[g, s, k],
            x, x_up, x_dn, x_far, lambda j: {"dp": j},
        )

    up_rings = [up_ring(g) for g in range(NG)]

    def up_part(g):
        rows = n_lat // n_x
        lhs = lat_all[pl.ds(rows_of[g] * 2, 2)].reshape(2 * n_lat, 2 * cap)
        step = 512
        for start in range(0, columns, step):
            rhs = g_v[:, :, start : start + step].reshape(2 * cap, step)
            part = dot(lhs, rhs, NN).astype(BF16)
            for k in range(2):
                for b in range(n_x):
                    at = k * n_lat + b * rows
                    u_b[g, b, k, :, start : start + step] = part[at : at + rows]
            if g == SWAPPED and (start + step) % half_c == 0:
                k = start // half_c
                ship(
                    u_b.at[g, :, 1 - parity, :, column_half(k)], u_pair.at[k],
                    {"mb": across_z[k]}, swap_pairs[g][k],
                )

    def up_swap():
        for k in range(2):
            arrive(u_pair.at[k], swap_pairs[SWAPPED][k])
            for b in range(n_x):
                both = u_b[SWAPPED, b, parity, :, column_half(k)].astype(F32) + u_pair[k, b].astype(F32)
                x_b[b, :, column_half(k)] = both.astype(BF16)

    def up_total(g):
        for k, part in enumerate(up_rings[g].total()):
            t_u[g, :, :, column_half(k)] = part.astype(BF16)
        for k in range(2):
            ship(
                t_u.at[g, 1 - parity, :, column_half(k)], t_pair.at[g, k],
                {"mb": across_z[k]}, swap_pairs[g][k],
            )

    up_hops = range(2, n_z, 2)
    up_base = sems.used
    up_pairs = [sems.take() for _ in up_hops]
    to_owner = []

    def up_owner(g):
        if g == SWAPPED:
            for k, part in enumerate(up_rings[g].total()):
                f_u[rows_of[g], :, column_half(k)] = part.astype(BF16)
        for k in range(2 if g != SWAPPED else 0):
            arrive(t_pair.at[g, k], swap_pairs[g][k])
            both = t_u[g, parity, :, column_half(k)].astype(F32) + t_pair[g, k].astype(F32)
            f_u[rows_of[g], :, column_half(k)] = both.astype(BF16)
        owner = 2 * rows_of[g] + parity
        hop = lax.rem(owner - z + n_z, n_z) // 2
        at = lax.rem(hop + n_z // 2 - 1, n_z // 2)
        slot = jnp.minimum(at, n_z // 2 - 2)
        copy = pltpu.make_async_remote_copy(
            src_ref=f_u.at[rows_of[g]], dst_ref=zr_u.at[slot],
            send_sem=send.at[up_base + slot], recv_sem=recv.at[up_base + slot],
            device_id={"mb": owner}, device_id_type=MESH,
        )
        pl.when(owner != z)(copy.start)
        own = pltpu.make_async_copy(f_u.at[rows_of[g]], zr_u.at[n_z // 2 - 1], save.at[2 * NH + g])
        pl.when(owner == z)(own.start)
        to_owner.append((owner, copy, own))

    def up_final():
        for d, pair in enumerate(up_pairs):
            arrive(zr_u.at[d], pair)

    cuts = [(h, lo, hi) for h in range(NH) for lo, hi in ((0, split), (split, width))]

    def down_ring(h, lo, hi):
        return ring_sum(
            lambda j, k: d_s[h, j, row_half(k, rx), lo:hi],
            lambda j, k: d_b.at[h, j, row_half(k, rx), lo:hi],
            lambda k: d_far.at[h, k, :, lo:hi],
            lambda s, k: d_near.at[h, s, k, :, lo:hi],
            x, x_up, x_dn, x_far, lambda j: {"dp": j},
        )

    down_rings = [down_ring(*cut) for cut in cuts]

    def down_part(i):
        h, lo, hi = cuts[i]
        lhs = lg_all[h]
        for start in range(lo, hi, 256):
            stop = min(start + 256, hi)
            part = dot(lhs, h_v[:, start:stop], NN)
            for j in range(n_x):
                rows = part[j * rx : (j + 1) * rx]
                d_s[h, j, :, start:stop] = rows
                d_b[h, j, :, start:stop] = rows.astype(BF16)

    out_pairs = [[sems.take() for _ in z_peers] for _ in cuts]
    back_pairs = [[sems.take() for _ in z_peers] for _ in cuts]

    def down_scatter(i):
        h, lo, hi = cuts[i]
        halves = down_rings[i].total()
        per_half = n_z // 2
        for k in range(2):
            zs_d[h, k * per_half : (k + 1) * per_half, :, lo:hi] = (
                halves[k].reshape(per_half, -1, hi - lo).astype(BF16)
            )
        zr_d[h, z, :, lo:hi] = zs_d[h, z, :, lo:hi]
        for p, pair in zip(z_peers, out_pairs[i]):
            ship(zs_d.at[h, p, :, lo:hi], zr_d.at[h, z, :, lo:hi], {"mb": p}, pair)

    def down_prefix(i):
        h, lo, hi = cuts[i]
        for p, pair in zip(z_sources, out_pairs[i]):
            arrive(zr_d.at[h, p, :, lo:hi], pair)
        total = zr_d[h, 0, :, lo:hi].astype(F32)
        po_d[h, 0, :, lo:hi] = total.astype(BF16)
        for p in range(1, n_z):
            total += zr_d[h, p, :, lo:hi].astype(F32)
            po_d[h, p, :, lo:hi] = total.astype(BF16)
        keep(po_d.at[h, z, :, lo:hi], rf_d.at[h, z, :, lo:hi])
        for p, pair in zip(z_peers, back_pairs[i]):
            ship(po_d.at[h, p, :, lo:hi], rf_d.at[h, z, :, lo:hi], {"mb": p}, pair)

    def down_arrive(i):
        h, lo, hi = cuts[i]
        for p, pair in zip(z_sources, back_pairs[i]):
            arrive(rf_d.at[h, p, :, lo:hi], pair)

    lat_gather.near()
    get_w[0].wait()
    get_g_other.wait()
    other_slot(0)
    get_g_own.wait()
    own_slot(0)
    get_w[1].wait()
    other_slot(1)
    pair_sum(0)
    lg_spread(0)
    lat_gather.finish(0)
    up_part(0)
    up_rings[0].far()
    up_rings[0].near()
    own_slot(1)
    pair_sum(1)
    lg_spread(1)
    lat_gather.across()
    lat_gather.finish(2)
    up_part(1)
    up_rings[1].far()
    lat_gather.finish(1)
    up_part(2)
    up_rings[0].second()
    up_rings[1].near()
    lg_final(0)
    lg_final(1)
    lat_gather.along()
    up_rings[1].second()
    up_total(0)
    lg_gathers[0].across_far()
    up_swap()
    up_rings[2].far()
    up_rings[2].near()
    lg_gathers[0].across()
    up_total(1)
    get_h.wait()
    lg_gathers[0].finish(0, 1, 2, 3)
    down_part(0)
    down_rings[0].far()
    down_part(1)
    down_rings[1].far()
    up_rings[2].second()
    down_rings[0].near()
    down_rings[1].near()
    up_owner(0)
    lg_gathers[1].across_far()
    lg_gathers[1].across()
    lg_gathers[1].finish(0, 1, 2, 3)
    down_part(2)
    down_rings[2].far()
    down_part(3)
    down_rings[3].far()
    up_owner(1)
    down_rings[0].second()
    down_rings[1].second()
    down_rings[2].near()
    down_rings[3].near()
    up_owner(2)
    lat_gather.across_halves()
    lat_gather.finish(3)
    up_part(3)
    down_rings[2].second()
    down_rings[3].second()
    up_rings[3].far()
    up_rings[3].near()
    down_scatter(0)
    down_scatter(1)
    down_scatter(2)
    down_scatter(3)
    up_rings[3].second()
    down_prefix(0)
    down_prefix(1)
    up_total(3)
    down_prefix(2)
    down_prefix(3)
    up_owner(3)
    down_arrive(0)
    down_arrive(1)
    down_arrive(2)
    down_arrive(3)
    up_final()
    for copy in sent:
        copy.wait_send()
    for copy in kept:
        copy.wait()
    for owner, copy, own in to_owner:
        pl.when(owner != z)(copy.wait_send)
        pl.when(owner == z)(own.wait)


def finish_kernel(up_in, down_in, up_out, down_out, up_v, down_v, up_w, down_w, load, save):
    loads = [
        pltpu.make_async_copy(src, dst, load.at[k])
        for k, (src, dst) in enumerate(((down_in, down_v), (up_in, up_v)))
    ]
    saves = [
        pltpu.make_async_copy(src, dst, save.at[k])
        for k, (src, dst) in enumerate(((down_w, down_out), (up_w, up_out)))
    ]
    for copy in loads:
        copy.start()
    loads[0].wait()
    down_w[...] = down_v[...].astype(F32).reshape(-1, down_v.shape[-1]).T
    saves[0].start()
    loads[1].wait()
    total = up_v[0].astype(F32)
    for k in range(1, up_v.shape[0]):
        total += up_v[k].astype(F32)
    up_w[...] = total
    saves[1].start()
    for copy in saves:
        copy.wait()


def local(sizes, hidden, latent, out_grad, up_weight, mb_tokens, slot_mb):
    n_z, n_y, n_x = sizes
    slot_count, cap, width = hidden.shape[1:]
    rank, columns = up_weight.shape
    n_lat = latent.shape[3]
    row_total = slot_count * cap
    rows_h = rank // NH
    rx = rows_h // n_x
    blk = cap // n_y
    rows_u = rank // n_x // n_z
    up_shape = (n_z // 2, rows_u, columns)
    down_shape = (NH, n_z, rx // n_z, width)
    in_hbm = pl.BlockSpec(memory_space=pltpu.HBM)
    n_sems = 8 + NH + 3 * NH + 8 * NH + 8 * NG + (n_z // 2 - 1) + 2 * (6 + 2 * (n_z - 1)) * NH
    up_grad, running = pl.pallas_call(
        functools.partial(kernel, n_z, n_y, n_x),
        out_shape=(
            jax.ShapeDtypeStruct(up_shape, BF16),
            jax.ShapeDtypeStruct(down_shape, BF16),
        ),
        in_specs=[in_hbm] * 6,
        out_specs=(in_hbm,) * 2,
        scratch_shapes=[
            pltpu.SMEM(mb_tokens.shape, jnp.int32),
            pltpu.SMEM(slot_mb.shape, jnp.int32),
            pltpu.VMEM((slot_count, n_lat, cap), BF16),
            pltpu.VMEM((row_total, width), BF16),
            pltpu.VMEM((slot_count, cap, columns), BF16),
            pltpu.VMEM((NH, n_x, rx, columns), BF16),
            pltpu.VMEM((2 * n_y, n_lat, row_total), BF16),
            pltpu.VMEM((NH, rows_h, cap), F32),
            pltpu.VMEM((NH, rows_h, cap), F32),
            pltpu.VMEM((NH, n_y, rows_h, blk), F32),
            pltpu.VMEM((NH, n_y, rows_h, blk), BF16),
            pltpu.VMEM((NH, 3, rows_h, blk), BF16),
            pltpu.VMEM((NH, rows_h, row_total), BF16),
            pltpu.VMEM((NH, n_x, rx, width), F32),
            pltpu.VMEM((NH, n_x, rx, width), BF16),
            pltpu.VMEM((NH, 2, rx // 2, width), BF16),
            pltpu.VMEM((NH, 2, 2, rx // 2, width), BF16),
            pltpu.VMEM(down_shape, BF16),
            pltpu.VMEM(down_shape, BF16),
            pltpu.VMEM(down_shape, BF16),
            pltpu.VMEM((NG, n_x, 2, rows_u, columns), BF16),
            pltpu.VMEM((2, n_x, rows_u, columns // 2), BF16),
            pltpu.VMEM((n_x, rows_u, columns), BF16),
            pltpu.VMEM((NG, 2, 2, rows_u, columns // 2), BF16),
            pltpu.VMEM((NG, 2, 2, 2, rows_u, columns // 2), BF16),
            pltpu.VMEM((NG, 2, rows_u, columns), BF16),
            pltpu.VMEM((NG, 2, rows_u, columns // 2), BF16),
            pltpu.VMEM((n_y, rows_u, columns), BF16),
            pltpu.SemaphoreType.DMA((10,)),
            pltpu.SemaphoreType.DMA((2 * NH + NG,)),
            pltpu.SemaphoreType.DMA((n_sems,)),
            pltpu.SemaphoreType.DMA((n_sems,)),
        ],
        compiler_params=pltpu.CompilerParams(
            collective_id=0, has_side_effects=True, vmem_limit_bytes=66_400_000
        ),
    )(
        hidden.reshape(row_total, width),
        latent[0].swapaxes(1, 2),
        out_grad.reshape(slot_count, cap, columns),
        up_weight.reshape(n_x, NH, rx, columns),
        mb_tokens,
        slot_mb,
    )
    up_grad, running = pl.pallas_call(
        finish_kernel,
        out_shape=(
            jax.ShapeDtypeStruct((rows_u, columns), F32),
            jax.ShapeDtypeStruct((width, rank // n_x), F32),
        ),
        in_specs=[in_hbm] * 2,
        out_specs=(in_hbm,) * 2,
        scratch_shapes=[
            pltpu.VMEM(up_shape, BF16),
            pltpu.VMEM(down_shape, BF16),
            pltpu.VMEM((rows_u, columns), F32),
            pltpu.VMEM((width, rank // n_x), F32),
            pltpu.SemaphoreType.DMA((2,)),
            pltpu.SemaphoreType.DMA((2,)),
        ],
        compiler_params=pltpu.CompilerParams(vmem_limit_bytes=66_400_000),
    )(up_grad, running)
    return up_grad, running[None]


def solution(mesh):
    sizes = (mesh.shape["mb"], mesh.shape["tp"] // 2, mesh.shape["dp"])
    return jax.shard_map(
        functools.partial(local, sizes),
        mesh=mesh,
        in_specs=(
            P("dp", "mb", None, "tp"),
            P("dp", "mb", None, "tp"),
            P("dp", "mb", None, "tp"),
            P(None, "tp"),
            P("dp", None),
            P("dp", "mb"),
        ),
        out_specs=(P(("mb", "dp"), "tp"), P("mb", "tp", "dp")),
        check_vma=False,
    )
```

```python
import collections
import functools

import jax
import jax.numpy as jnp
from jax import lax
from jax.experimental import pallas as pl
from jax.experimental.pallas import tpu as pltpu
from jax.sharding import PartitionSpec as P

MESH = pl.DeviceIdType.MESH
F32 = jnp.float32
BF16 = jnp.bfloat16
NT = (((1,), (1,)), ((), ()))
NN = (((1,), (0,)), ((), ()))
NH = 2
SWAPPED = (2,)
NG = 4


def dot(a, b, dims):
    return lax.dot_general(a, b, dims, preferred_element_type=F32)


Gather = collections.namedtuple(
    "Gather", ["near", "across", "along", "across_halves", "far", "across_far", "finish"]
)
Ring = collections.namedtuple("Ring", ["far", "near", "second", "total"])


class Sems:
    def __init__(self, send, recv):
        self.send, self.recv, self.used = send, recv, [0, 0]

    def take(self, sends=1, recvs=1):
        sends = self.send.at[self.used[0]] if sends else None
        recvs = self.recv.at[self.used[1]] if recvs else None
        self.used[0] += sends is not None
        self.used[1] += recvs is not None
        return sends, recvs


def kernel(
    n_z, n_y, n_x,
    hidden, latent, out_grad, weight, tokens_in, slots_in,
    zr_u, rf_d,
    tokens, slots,
    lat_v, h_v, g_v, w_v, lat_all,
    pair_s, pair_r, lg_s, lg_b, lg_in, lg_all,
    d_s, d_b, d_far, d_near, zs_d, zr_d, po_d,
    u_b, u_pair, x_b, u_far, u_near, t_u, t_pair, f_u,
    load, save, send, recv,
):
    z = lax.axis_index("mb")
    tp = lax.axis_index("tp")
    x = lax.axis_index("dp")
    y, c = tp // 2, tp % 2
    oc = 1 - c
    cap = g_v.shape[1]
    blk = cap // n_y
    rows_h = lg_all.shape[1]
    rx = rows_h // n_x
    width = h_v.shape[1]
    columns = g_v.shape[2]
    half_c = columns // 2
    split = (width // 2 + 127) // 128 * 128

    def tp_of(row, core):
        return lax.rem(row + 2 * n_y, n_y) * 2 + core

    y_up, y_dn, y_far = tp_of(y + 1, c), tp_of(y - 1, c), tp_of(y + 2, c)
    x_up, x_dn, x_far = lax.rem(x + 1, n_x), lax.rem(x + n_x - 1, n_x), lax.rem(x + 2, n_x)
    partner = tp_of(y, oc)
    peers = [{"tp": partner}, {"tp": y_up}, {"tp": y_dn}]
    peers += [{"tp": y_far}]
    peers += [{"dp": x_up}, {"dp": x_dn}]
    hops = sorted(range(1, n_z), key=lambda d: -min(d, n_z - d))
    z_peers = [lax.rem(z + d, n_z) for d in hops]
    peers += [{"mb": p} for p in z_peers]

    loads = []

    def fetch(src, dst):
        copy = pltpu.make_async_copy(src, dst, load.at[len(loads)])
        copy.start()
        loads.append(copy)
        return copy

    barrier = pltpu.get_barrier_semaphore()
    for peer in peers:
        pl.semaphore_signal(barrier, inc=1, device_id=peer, device_id_type=MESH)
    get_lat = fetch(latent, lat_v)
    get_scalars = [fetch(tokens_in, tokens), fetch(slots_in, slots)]
    get_w = [fetch(weight.at[:, 0], w_v.at[0])]
    get_g_other = fetch(out_grad.at[oc], g_v.at[oc])
    get_g_own = fetch(out_grad.at[c], g_v.at[c])
    get_w += [fetch(weight.at[:, h], w_v.at[h]) for h in range(1, NH)]
    get_h = fetch(hidden, h_v)

    sent = []
    kept = []
    sems = Sems(send, recv)

    def keep(src, dst):
        copy = pltpu.make_async_copy(src, dst, save.at[len(kept)])
        copy.start()
        kept.append(copy)

    drains = []

    def ship(src, dst, device, pair, drain=True):
        copy = pltpu.make_async_remote_copy(
            src_ref=src, dst_ref=dst, send_sem=pair[0], recv_sem=pair[1],
            device_id=device, device_id_type=MESH,
        )
        copy.start()
        if drain:
            sent.append(copy)

    def arrive(dst, pair):
        pltpu.make_async_remote_copy(
            src_ref=dst, dst_ref=dst, send_sem=send.at[0], recv_sem=pair[1],
            device_id={"tp": partner}, device_id_type=MESH,
        ).wait_recv()

    for copy in get_scalars:
        copy.wait()
    count = [tokens[0, slots[0, s]] for s in range(2)]

    get_lat.wait()
    n_lat = lat_v.shape[1]
    for s in range(2):
        part = lat_v[s].astype(F32)
        position = lax.broadcasted_iota(jnp.int32, part.shape, 1)
        part = jnp.where(position < count[s], part, 0.0).astype(BF16)
        lat_all[tp, :, s * cap : (s + 1) * cap] = part
    pl.semaphore_wait(barrier, len(peers))

    def row_half(k, rows):
        return pl.ds(k * rows // 2, rows // 2)

    def gather(block, half):
        pairs = [sems.take() for _ in range(8)]

        def near():
            ship(block(tp), block(tp), {"tp": y_up}, pairs[0])
            ship(block(tp), block(tp), {"tp": y_dn}, pairs[1])
            ship(block(tp), block(tp), {"tp": partner}, pairs[2])

        def across():
            arrive(block(y_dn), pairs[0])
            ship(block(y_dn), block(y_dn), {"tp": partner}, pairs[5])
            arrive(block(y_up), pairs[1])
            ship(block(y_up), block(y_up), {"tp": partner}, pairs[6])

        def along():
            ship(half(y_dn, 0), half(y_dn, 0), {"tp": y_up}, pairs[3])
            ship(half(y_up, 1), half(y_up, 1), {"tp": y_dn}, pairs[4])

        def across_halves():
            arrive(half(y_far, 0), pairs[3])
            arrive(half(y_far, 1), pairs[4])
            ship(block(y_far), block(y_far), {"tp": partner}, pairs[7])

        def far():
            ship(block(tp), block(tp), {"tp": y_far}, pairs[3])

        def across_far():
            arrive(block(y_far), pairs[3])
            ship(block(y_far), block(y_far), {"tp": partner}, pairs[7])

        def finish(*which):
            for k in which:
                arrive(block(tp_of(y + (0, -1, 1, 2)[k], oc)), pairs[(2, 5, 6, 7)[k]])

        return Gather(near, across, along, across_halves, far, across_far, finish)

    def ring_sum(value, block, far, near, three, me, up, dn, across, device):
        out, in_far, in_near = sems.take(1, 0), sems.take(0, 1), sems.take(0, 1)
        to_far, to_near = (out[0], in_far[1]), (out[0], in_near[1])
        drains.append((three, out))

        def send_far():
            ship(block(across, 0), far(0), device(up), to_far, False)
            ship(block(across, 1), far(1), device(dn), to_far, False)

        def send_near():
            ship(block(up, 1), near(0, 1), device(up), to_near, False)
            ship(block(dn, 0), near(1, 0), device(dn), to_near, False)

        def second():
            arrive(far(None), in_far)
            block(up, 0)[...] = (value(up, 0) + far(0)[...].astype(F32)).astype(BF16)
            ship(block(up, 0), near(0, 0), device(up), to_near, False)
            block(dn, 1)[...] = (value(dn, 1) + far(1)[...].astype(F32)).astype(BF16)
            ship(block(dn, 1), near(1, 1), device(dn), to_near, False)

        def total():
            arrive(near(None, None), in_near)
            return [
                value(me, k) + near(0, k)[...].astype(F32) + near(1, k)[...].astype(F32)
                for k in range(2)
            ]

        return Ring(send_far, send_near, second, total)

    lat_gather = gather(
        lambda i: lat_all.at[i],
        lambda i, k: lat_all.at[i, row_half(k, n_lat)],
    )

    pair_pairs = [sems.take() for _ in range(NH)]

    def weights(h):
        return w_v[h].reshape(rows_h, columns)

    def other_slot(h):
        pair_s[h] = dot(weights(h), g_v[oc], NT)
        ship(pair_s.at[h], pair_r.at[h], {"tp": partner}, pair_pairs[h])

    def own_slot(h):
        part = dot(weights(h), g_v[c], NT)
        for j in range(n_y):
            lg_s[h, j] = part[:, j * blk : (j + 1) * blk]

    def pair_sum(h):
        arrive(pair_r.at[h], pair_pairs[h])
        for j in range(n_y):
            both = lg_s[h, j] + pair_r[h, :, j * blk : (j + 1) * blk]
            lg_s[h, j] = both
            lg_b[h, j] = both.astype(BF16)

    lg_hops = (2, 1, n_y - 1)
    lg_pairs = [[sems.take() for _ in lg_hops] for _ in range(NH)]

    def lg_spread(h):
        for k, hop in enumerate(lg_hops):
            row = lax.rem(y + hop, n_y)
            ship(lg_b.at[h, row], lg_in.at[h, k], {"tp": row * 2 + c}, lg_pairs[h][k])

    def lg_gather(h):
        def columns_of(i):
            start = pl.multiple_of(lax.rem(i, 2) * cap + (i // 2) * blk, blk)
            return pl.ds(start, blk)

        return gather(
            lambda i: lg_all.at[h, :, columns_of(i)],
            lambda i, k: lg_all.at[h, row_half(k, rows_h), columns_of(i)],
        )

    lg_gathers = [lg_gather(h) for h in range(NH)]
    live = jnp.where(c == 0, count[0], count[1]) > y * blk

    def lg_final(h):
        total = lg_s[h, y]
        for k in range(len(lg_hops)):
            arrive(lg_in.at[h, k], lg_pairs[h][k])
            total += lg_in[h, k].astype(F32)
        start = pl.multiple_of(c * cap + y * blk, blk)
        lg_all[h, :, pl.ds(start, blk)] = jnp.where(live, total, 0.0).astype(BF16)
        lg_gathers[h].far()
        lg_gathers[h].near()

    rows_of = [lax.rem(y + n_y + off, n_y) for off in (0, 1, -1, 2)]
    parity = lax.rem(z, 2)
    across_z = [lax.rem(z + n_z + 1 - 2 * lax.rem(z + k, 2), n_z) for k in range(2)]
    swap_pairs = [[sems.take() for _ in range(2)] for _ in range(NG)]

    def column_half(k):
        return pl.ds(k * half_c, half_c)

    def up_ring(g):
        if g in SWAPPED:
            at = SWAPPED.index(g)
            return ring_sum(
                lambda j, k: x_b[at, j, :, column_half(k)].astype(F32),
                lambda j, k: x_b.at[at, j, :, column_half(k)],
                lambda k: u_far.at[g, :, 0] if k is None else u_far.at[g, k, 0],
                lambda s, k: u_near.at[g, :, :, 0] if s is None else u_near.at[g, s, k, 0],
                x_b.at[at, 0:3],
                x, x_up, x_dn, x_far, lambda j: {"dp": j},
            )
        return ring_sum(
            lambda j, k: u_b[g, j, :, :, column_half(k)].astype(F32),
            lambda j, k: u_b.at[g, j, :, :, column_half(k)],
            lambda k: u_far.at[g] if k is None else u_far.at[g, k],
            lambda s, k: u_near.at[g] if s is None else u_near.at[g, s, k],
            u_b.at[g, 0:3],
            x, x_up, x_dn, x_far, lambda j: {"dp": j},
        )

    up_rings = [up_ring(g) for g in range(NG)]

    def up_part(g):
        rows = n_lat // n_x
        lhs = lat_all[pl.ds(rows_of[g] * 2, 2)].reshape(2 * n_lat, 2 * cap)
        step = 512
        for start in range(0, columns, step):
            rhs = g_v[:, :, start : start + step].reshape(2 * cap, step)
            part = dot(lhs, rhs, NN).astype(BF16)
            for k in range(2):
                for b in range(n_x):
                    at = k * n_lat + b * rows
                    u_b[g, b, k, :, start : start + step] = part[at : at + rows]
            if g in SWAPPED and (start + step) % half_c == 0:
                k = start // half_c
                ship(
                    u_b.at[g, :, 1 - parity, :, column_half(k)], u_pair.at[SWAPPED.index(g), k],
                    {"mb": across_z[k]}, swap_pairs[g][k],
                )

    def up_swap(g):
        at = SWAPPED.index(g)
        for k in range(2):
            arrive(u_pair.at[at, k], swap_pairs[g][k])
            for b in range(n_x):
                both = u_b[g, b, parity, :, column_half(k)].astype(F32) + u_pair[at, k, b].astype(F32)
                x_b[at, b, :, column_half(k)] = both.astype(BF16)

    def up_total(g):
        for k, part in enumerate(up_rings[g].total()):
            t_u[g, :, :, column_half(k)] = part.astype(BF16)
        for k in range(2):
            ship(
                t_u.at[g, 1 - parity, :, column_half(k)], t_pair.at[g, k],
                {"mb": across_z[k]}, swap_pairs[g][k],
            )

    up_hops = range(2, n_z, 2)
    up_base = list(sems.used)
    up_pairs = [sems.take() for _ in up_hops]
    to_owner = []

    def up_owner(g):
        if g in SWAPPED:
            for k, part in enumerate(up_rings[g].total()):
                f_u[rows_of[g], :, column_half(k)] = part.astype(BF16)
        for k in range(2 if g not in SWAPPED else 0):
            arrive(t_pair.at[g, k], swap_pairs[g][k])
            both = t_u[g, parity, :, column_half(k)].astype(F32) + t_pair[g, k].astype(F32)
            f_u[rows_of[g], :, column_half(k)] = both.astype(BF16)
        owner = 2 * rows_of[g] + parity
        hop = lax.rem(owner - z + n_z, n_z) // 2
        at = lax.rem(hop + n_z // 2 - 1, n_z // 2)
        slot = jnp.minimum(at, n_z // 2 - 2)
        copy = pltpu.make_async_remote_copy(
            src_ref=f_u.at[rows_of[g]], dst_ref=zr_u.at[slot],
            send_sem=send.at[up_base[0] + slot], recv_sem=recv.at[up_base[1] + slot],
            device_id={"mb": owner}, device_id_type=MESH,
        )
        pl.when(owner != z)(copy.start)
        own = pltpu.make_async_copy(f_u.at[rows_of[g]], zr_u.at[n_z // 2 - 1], save.at[2 * NH + g])
        pl.when(owner == z)(own.start)
        to_owner.append((owner, copy, own))

    def up_final():
        for d, pair in enumerate(up_pairs):
            arrive(zr_u.at[d], pair)

    cuts = [(h, lo, hi) for h in range(NH) for lo, hi in ((0, split), (split, width))]

    def down_ring(h, lo, hi):
        return ring_sum(
            lambda j, k: d_s[h, j, row_half(k, rx), lo:hi],
            lambda j, k: d_b.at[h, j, row_half(k, rx), lo:hi],
            lambda k: d_far.at[h, :, :, lo:hi] if k is None else d_far.at[h, k, :, lo:hi],
            lambda s, k: (
                d_near.at[h, :, :, :, lo:hi] if s is None else d_near.at[h, s, k, :, lo:hi]
            ),
            d_b.at[h, 0:3, :, lo:hi],
            x, x_up, x_dn, x_far, lambda j: {"dp": j},
        )

    down_rings = [down_ring(*cut) for cut in cuts]

    def down_part(i):
        h, lo, hi = cuts[i]
        lhs = lg_all[h]
        for start in range(lo, hi, 256):
            stop = min(start + 256, hi)
            part = dot(lhs, h_v[:, start:stop], NN)
            for j in range(n_x):
                rows = part[j * rx : (j + 1) * rx]
                d_s[h, j, :, start:stop] = rows
                d_b[h, j, :, start:stop] = rows.astype(BF16)

    def all_but_one(ref, i):
        h, lo, hi = cuts[i]
        return ref.at[h, 0 : n_z - 1, :, lo:hi]

    out_pairs = [sems.take() for _ in cuts]
    back_pairs = [sems.take() for _ in cuts]
    for i in range(len(cuts)):
        drains.append((all_but_one(zs_d, i), out_pairs[i]))
        drains.append((all_but_one(po_d, i), back_pairs[i]))

    def down_scatter(i):
        h, lo, hi = cuts[i]
        halves = down_rings[i].total()
        per_half = n_z // 2
        for k in range(2):
            zs_d[h, k * per_half : (k + 1) * per_half, :, lo:hi] = (
                halves[k].reshape(per_half, -1, hi - lo).astype(BF16)
            )
        zr_d[h, z, :, lo:hi] = zs_d[h, z, :, lo:hi]
        for p in z_peers:
            ship(zs_d.at[h, p, :, lo:hi], zr_d.at[h, z, :, lo:hi], {"mb": p}, out_pairs[i], False)

    def down_prefix(i):
        h, lo, hi = cuts[i]
        arrive(all_but_one(zr_d, i), out_pairs[i])
        total = zr_d[h, 0, :, lo:hi].astype(F32)
        po_d[h, 0, :, lo:hi] = total.astype(BF16)
        for p in range(1, n_z):
            total += zr_d[h, p, :, lo:hi].astype(F32)
            po_d[h, p, :, lo:hi] = total.astype(BF16)
        keep(po_d.at[h, z, :, lo:hi], rf_d.at[h, z, :, lo:hi])
        for p in z_peers:
            ship(po_d.at[h, p, :, lo:hi], rf_d.at[h, z, :, lo:hi], {"mb": p}, back_pairs[i], False)

    def down_arrive(i):
        arrive(all_but_one(rf_d, i), back_pairs[i])

    assert sems.used == [send.shape[0], recv.shape[0]], sems.used
    lat_gather.near()
    get_w[0].wait()
    get_g_other.wait()
    other_slot(0)
    get_g_own.wait()
    own_slot(0)
    get_w[1].wait()
    other_slot(1)
    pair_sum(0)
    lg_spread(0)
    lat_gather.finish(0)
    up_part(0)
    up_rings[0].far()
    up_rings[0].near()
    own_slot(1)
    pair_sum(1)
    lg_spread(1)
    lat_gather.across()
    lat_gather.finish(2)
    up_part(1)
    up_rings[1].far()
    lat_gather.finish(1)
    up_part(2)
    up_rings[0].second()
    up_rings[1].near()
    lg_final(0)
    lg_final(1)
    lat_gather.along()
    up_rings[1].second()
    up_total(0)
    lg_gathers[0].across_far()
    up_swap(2)
    up_rings[2].far()
    up_rings[2].near()
    lg_gathers[0].across()
    up_total(1)
    get_h.wait()
    lg_gathers[0].finish(0, 1, 2, 3)
    lg_gathers[1].across_far()
    down_part(0)
    down_rings[0].far()
    down_part(1)
    down_rings[1].far()
    lg_gathers[1].across()
    up_rings[2].second()
    down_rings[0].near()
    down_rings[1].near()
    up_owner(0)
    lg_gathers[1].finish(0, 1, 2, 3)
    lat_gather.across_halves()
    down_part(2)
    down_rings[2].far()
    down_part(3)
    down_rings[3].far()
    lat_gather.finish(3)
    up_part(3)
    down_rings[0].second()
    down_rings[1].second()
    down_rings[2].near()
    down_rings[3].near()
    up_owner(1)
    up_owner(2)
    down_rings[2].second()
    down_rings[3].second()
    up_rings[3].far()
    up_rings[3].near()
    down_scatter(0)
    down_scatter(1)
    down_scatter(2)
    down_scatter(3)
    up_rings[3].second()
    down_prefix(0)
    down_prefix(1)
    up_total(3)
    down_prefix(2)
    down_prefix(3)
    up_owner(3)
    down_arrive(0)
    down_arrive(1)
    down_arrive(2)
    down_arrive(3)
    up_final()
    for copy in sent:
        copy.wait_send()
    for whole, pair in drains:
        pltpu.make_async_remote_copy(
            src_ref=whole, dst_ref=whole, send_sem=pair[0], recv_sem=recv.at[0],
            device_id={"tp": partner}, device_id_type=MESH,
        ).wait_send()
    for copy in kept:
        copy.wait()
    for owner, copy, own in to_owner:
        pl.when(owner != z)(copy.wait_send)
        pl.when(owner == z)(own.wait)


def finish_kernel(up_in, down_in, up_out, down_out, up_v, down_v, up_w, down_w, load, save):
    loads = [
        pltpu.make_async_copy(src, dst, load.at[k])
        for k, (src, dst) in enumerate(((down_in, down_v), (up_in, up_v)))
    ]
    saves = [
        pltpu.make_async_copy(src, dst, save.at[k])
        for k, (src, dst) in enumerate(((down_w, down_out), (up_w, up_out)))
    ]
    for copy in loads:
        copy.start()
    loads[0].wait()
    down_w[...] = down_v[...].astype(F32).reshape(-1, down_v.shape[-1]).T
    saves[0].start()
    loads[1].wait()
    total = up_v[0].astype(F32)
    for k in range(1, up_v.shape[0]):
        total += up_v[k].astype(F32)
    up_w[...] = total
    saves[1].start()
    for copy in saves:
        copy.wait()


def local(sizes, hidden, latent, out_grad, up_weight, mb_tokens, slot_mb):
    n_z, n_y, n_x = sizes
    slot_count, cap, width = hidden.shape[1:]
    rank, columns = up_weight.shape
    n_lat = latent.shape[3]
    row_total = slot_count * cap
    rows_h = rank // NH
    rx = rows_h // n_x
    blk = cap // n_y
    rows_u = rank // n_x // n_z
    up_shape = (n_z // 2, rows_u, columns)
    down_shape = (NH, n_z, rx // n_z, width)
    in_hbm = pl.BlockSpec(memory_space=pltpu.HBM)
    both = 8 + NH + 3 * NH + 8 * NH + 2 * NG + (n_z // 2 - 1) + 2 * 2 * NH
    n_send, n_recv = both + NG + 2 * NH, both + 2 * NG + 2 * 2 * NH
    up_grad, running = pl.pallas_call(
        functools.partial(kernel, n_z, n_y, n_x),
        out_shape=(
            jax.ShapeDtypeStruct(up_shape, BF16),
            jax.ShapeDtypeStruct(down_shape, BF16),
        ),
        in_specs=[in_hbm] * 6,
        out_specs=(in_hbm,) * 2,
        scratch_shapes=[
            pltpu.SMEM(mb_tokens.shape, jnp.int32),
            pltpu.SMEM(slot_mb.shape, jnp.int32),
            pltpu.VMEM((slot_count, n_lat, cap), BF16),
            pltpu.VMEM((row_total, width), BF16),
            pltpu.VMEM((slot_count, cap, columns), BF16),
            pltpu.VMEM((NH, n_x, rx, columns), BF16),
            pltpu.VMEM((2 * n_y, n_lat, row_total), BF16),
            pltpu.VMEM((NH, rows_h, cap), F32),
            pltpu.VMEM((NH, rows_h, cap), F32),
            pltpu.VMEM((NH, n_y, rows_h, blk), F32),
            pltpu.VMEM((NH, n_y, rows_h, blk), BF16),
            pltpu.VMEM((NH, 3, rows_h, blk), BF16),
            pltpu.VMEM((NH, rows_h, row_total), BF16),
            pltpu.VMEM((NH, n_x, rx, width), F32),
            pltpu.VMEM((NH, n_x, rx, width), BF16),
            pltpu.VMEM((NH, 2, rx // 2, width), BF16),
            pltpu.VMEM((NH, 2, 2, rx // 2, width), BF16),
            pltpu.VMEM(down_shape, BF16),
            pltpu.VMEM(down_shape, BF16),
            pltpu.VMEM(down_shape, BF16),
            pltpu.VMEM((NG, n_x, 2, rows_u, columns), BF16),
            pltpu.VMEM((len(SWAPPED), 2, n_x, rows_u, columns // 2), BF16),
            pltpu.VMEM((len(SWAPPED), n_x, rows_u, columns), BF16),
            pltpu.VMEM((NG, 2, 2, rows_u, columns // 2), BF16),
            pltpu.VMEM((NG, 2, 2, 2, rows_u, columns // 2), BF16),
            pltpu.VMEM((NG, 2, rows_u, columns), BF16),
            pltpu.VMEM((NG, 2, rows_u, columns // 2), BF16),
            pltpu.VMEM((n_y, rows_u, columns), BF16),
            pltpu.SemaphoreType.DMA((6 + NH,)),
            pltpu.SemaphoreType.DMA((2 * NH + NG,)),
            pltpu.SemaphoreType.DMA((n_send,)),
            pltpu.SemaphoreType.DMA((n_recv,)),
        ],
        compiler_params=pltpu.CompilerParams(
            collective_id=0, has_side_effects=True, vmem_limit_bytes=66_400_000
        ),
    )(
        hidden.reshape(row_total, width),
        latent[0].swapaxes(1, 2),
        out_grad.reshape(slot_count, cap, columns),
        up_weight.reshape(n_x, NH, rx, columns),
        mb_tokens,
        slot_mb,
    )
    up_grad, running = pl.pallas_call(
        finish_kernel,
        out_shape=(
            jax.ShapeDtypeStruct((rows_u, columns), F32),
            jax.ShapeDtypeStruct((width, rank // n_x), F32),
        ),
        in_specs=[in_hbm] * 2,
        out_specs=(in_hbm,) * 2,
        scratch_shapes=[
            pltpu.VMEM(up_shape, BF16),
            pltpu.VMEM(down_shape, BF16),
            pltpu.VMEM((rows_u, columns), F32),
            pltpu.VMEM((width, rank // n_x), F32),
            pltpu.SemaphoreType.DMA((2,)),
            pltpu.SemaphoreType.DMA((2,)),
        ],
        compiler_params=pltpu.CompilerParams(vmem_limit_bytes=66_400_000),
    )(up_grad, running)
    return up_grad, running[None]


def solution(mesh):
    sizes = (mesh.shape["mb"], mesh.shape["tp"] // 2, mesh.shape["dp"])
    return jax.shard_map(
        functools.partial(local, sizes),
        mesh=mesh,
        in_specs=(
            P("dp", "mb", None, "tp"),
            P("dp", "mb", None, "tp"),
            P("dp", "mb", None, "tp"),
            P(None, "tp"),
            P("dp", None),
            P("dp", "mb"),
        ),
        out_specs=(P(("mb", "dp"), "tp"), P("mb", "tp", "dp")),
        check_vma=False,
    )
```

```python
import collections
import functools

import jax
import jax.numpy as jnp
from jax import lax
from jax.experimental import pallas as pl
from jax.experimental.pallas import tpu as pltpu
from jax.sharding import PartitionSpec as P

MESH = pl.DeviceIdType.MESH
F32 = jnp.float32
BF16 = jnp.bfloat16
NT = (((1,), (1,)), ((), ()))
NN = (((1,), (0,)), ((), ()))
NH = 2
SWAPPED = (2,)
NG = 4


def dot(a, b, dims):
    return lax.dot_general(a, b, dims, preferred_element_type=F32)


Gather = collections.namedtuple(
    "Gather", ["near", "across", "along", "across_halves", "far", "across_far", "finish"]
)
Ring = collections.namedtuple("Ring", ["far", "near", "second", "total"])


class Sems:
    def __init__(self, send, recv):
        self.send, self.recv, self.used = send, recv, [0, 0]

    def take(self, sends=1, recvs=1):
        sends = self.send.at[self.used[0]] if sends else None
        recvs = self.recv.at[self.used[1]] if recvs else None
        self.used[0] += sends is not None
        self.used[1] += recvs is not None
        return sends, recvs


def kernel(
    n_z, n_y, n_x,
    hidden, latent, out_grad, weight, tokens_in, slots_in,
    zr_u, rf_d,
    tokens, slots,
    lat_v, h_v, g_v, w_v, lat_all,
    pair_s, pair_r, lg_s, lg_b, lg_in, lg_all,
    d_s, d_b, d_far, d_near, zs_d, zr_d, po_d,
    u_b, u_pair, x_b, u_far, u_near, t_u, t_pair, f_u,
    load, save, send, recv,
):
    z = lax.axis_index("mb")
    tp = lax.axis_index("tp")
    x = lax.axis_index("dp")
    y, c = tp // 2, tp % 2
    oc = 1 - c
    cap = g_v.shape[1]
    blk = cap // n_y
    rows_h = lg_all.shape[1]
    rx = rows_h // n_x
    width = h_v.shape[1]
    columns = g_v.shape[2]
    half_c = columns // 2
    split = (width // 2 + 127) // 128 * 128

    def tp_of(row, core):
        return lax.rem(row + 2 * n_y, n_y) * 2 + core

    y_up, y_dn, y_far = tp_of(y + 1, c), tp_of(y - 1, c), tp_of(y + 2, c)
    x_up, x_dn, x_far = lax.rem(x + 1, n_x), lax.rem(x + n_x - 1, n_x), lax.rem(x + 2, n_x)
    partner = tp_of(y, oc)
    peers = [{"tp": partner}, {"tp": y_up}, {"tp": y_dn}]
    peers += [{"tp": y_far}]
    peers += [{"dp": x_up}, {"dp": x_dn}]
    hops = sorted(range(1, n_z), key=lambda d: -min(d, n_z - d))
    z_peers = [lax.rem(z + d, n_z) for d in hops]
    peers += [{"mb": p} for p in z_peers]

    loads = []

    def fetch(src, dst):
        copy = pltpu.make_async_copy(src, dst, load.at[len(loads)])
        copy.start()
        loads.append(copy)
        return copy

    barrier = pltpu.get_barrier_semaphore()
    for peer in peers:
        pl.semaphore_signal(barrier, inc=1, device_id=peer, device_id_type=MESH)
    get_lat = fetch(latent, lat_v)
    get_scalars = [fetch(tokens_in, tokens), fetch(slots_in, slots)]
    get_w = [fetch(weight.at[:, 0], w_v.at[0])]
    get_g_other = fetch(out_grad.at[oc], g_v.at[oc])
    get_g_own = fetch(out_grad.at[c], g_v.at[c])
    get_w += [fetch(weight.at[:, h], w_v.at[h]) for h in range(1, NH)]
    get_h = fetch(hidden, h_v)

    sent = []
    kept = []
    sems = Sems(send, recv)

    def keep(src, dst):
        copy = pltpu.make_async_copy(src, dst, save.at[len(kept)])
        copy.start()
        kept.append(copy)

    drains = []

    def ship(src, dst, device, pair, drain=True):
        copy = pltpu.make_async_remote_copy(
            src_ref=src, dst_ref=dst, send_sem=pair[0], recv_sem=pair[1],
            device_id=device, device_id_type=MESH,
        )
        copy.start()
        if drain:
            sent.append(copy)

    def arrive(dst, pair):
        pltpu.make_async_remote_copy(
            src_ref=dst, dst_ref=dst, send_sem=send.at[0], recv_sem=pair[1],
            device_id={"tp": partner}, device_id_type=MESH,
        ).wait_recv()

    for copy in get_scalars:
        copy.wait()
    count = [tokens[0, slots[0, s]] for s in range(2)]

    get_lat.wait()
    n_lat = lat_v.shape[1]
    for s in range(2):
        part = lat_v[s].astype(F32)
        position = lax.broadcasted_iota(jnp.int32, part.shape, 1)
        part = jnp.where(position < count[s], part, 0.0).astype(BF16)
        lat_all[tp, :, s * cap : (s + 1) * cap] = part
    pl.semaphore_wait(barrier, len(peers))

    def row_half(k, rows):
        return pl.ds(k * rows // 2, rows // 2)

    def gather(block, half, seven):
        out = sems.take(1, 0)
        drains.append((seven, out))
        pairs = [(out[0], sems.take(0, 1)[1]) for _ in range(8)]

        def near():
            ship(block(tp), block(tp), {"tp": y_up}, pairs[0], False)
            ship(block(tp), block(tp), {"tp": y_dn}, pairs[1], False)
            ship(block(tp), block(tp), {"tp": partner}, pairs[2], False)

        def across():
            arrive(block(y_dn), pairs[0])
            ship(block(y_dn), block(y_dn), {"tp": partner}, pairs[5], False)
            arrive(block(y_up), pairs[1])
            ship(block(y_up), block(y_up), {"tp": partner}, pairs[6], False)

        def along():
            ship(half(y_dn, 0), half(y_dn, 0), {"tp": y_up}, pairs[3], False)
            ship(half(y_up, 1), half(y_up, 1), {"tp": y_dn}, pairs[4], False)

        def across_halves():
            arrive(half(y_far, 0), pairs[3])
            arrive(half(y_far, 1), pairs[4])
            ship(block(y_far), block(y_far), {"tp": partner}, pairs[7], False)

        def far():
            ship(block(tp), block(tp), {"tp": y_far}, pairs[3], False)

        def across_far():
            arrive(block(y_far), pairs[3])
            ship(block(y_far), block(y_far), {"tp": partner}, pairs[7], False)

        def finish(*which):
            for k in which:
                arrive(block(tp_of(y + (0, -1, 1, 2)[k], oc)), pairs[(2, 5, 6, 7)[k]])

        return Gather(near, across, along, across_halves, far, across_far, finish)

    def ring_sum(value, block, far, near, three, me, up, dn, across, device):
        out, in_far, in_near = sems.take(1, 0), sems.take(0, 1), sems.take(0, 1)
        to_far, to_near = (out[0], in_far[1]), (out[0], in_near[1])
        drains.append((three, out))

        def send_far():
            ship(block(across, 0), far(0), device(up), to_far, False)
            ship(block(across, 1), far(1), device(dn), to_far, False)

        def send_near():
            ship(block(up, 1), near(0, 1), device(up), to_near, False)
            ship(block(dn, 0), near(1, 0), device(dn), to_near, False)

        def second():
            arrive(far(None), in_far)
            block(up, 0)[...] = (value(up, 0) + far(0)[...].astype(F32)).astype(BF16)
            ship(block(up, 0), near(0, 0), device(up), to_near, False)
            block(dn, 1)[...] = (value(dn, 1) + far(1)[...].astype(F32)).astype(BF16)
            ship(block(dn, 1), near(1, 1), device(dn), to_near, False)

        def total():
            arrive(near(None, None), in_near)
            return [
                value(me, k) + near(0, k)[...].astype(F32) + near(1, k)[...].astype(F32)
                for k in range(2)
            ]

        return Ring(send_far, send_near, second, total)

    lat_gather = gather(
        lambda i: lat_all.at[i],
        lambda i, k: lat_all.at[i, row_half(k, n_lat)],
        lat_all.at[0:7],
    )

    pair_pairs = [sems.take() for _ in range(NH)]

    def weights(h):
        return w_v[h].reshape(rows_h, columns)

    def other_slot(h):
        pair_s[h] = dot(weights(h), g_v[oc], NT)
        ship(pair_s.at[h], pair_r.at[h], {"tp": partner}, pair_pairs[h])

    def own_slot(h):
        part = dot(weights(h), g_v[c], NT)
        for j in range(n_y):
            lg_s[h, j] = part[:, j * blk : (j + 1) * blk]

    def pair_sum(h):
        arrive(pair_r.at[h], pair_pairs[h])
        for j in range(n_y):
            both = lg_s[h, j] + pair_r[h, :, j * blk : (j + 1) * blk]
            lg_s[h, j] = both
            lg_b[h, j] = both.astype(BF16)

    lg_hops = (2, 1, n_y - 1)
    lg_pairs = [[sems.take() for _ in lg_hops] for _ in range(NH)]

    def lg_spread(h):
        for k, hop in enumerate(lg_hops):
            row = lax.rem(y + hop, n_y)
            ship(lg_b.at[h, row], lg_in.at[h, k], {"tp": row * 2 + c}, lg_pairs[h][k])

    def lg_gather(h):
        def columns_of(i):
            start = pl.multiple_of(lax.rem(i, 2) * cap + (i // 2) * blk, blk)
            return pl.ds(start, blk)

        return gather(
            lambda i: lg_all.at[h, :, columns_of(i)],
            lambda i, k: lg_all.at[h, row_half(k, rows_h), columns_of(i)],
            lg_all.at[h, :, 0 : 7 * blk],
        )

    lg_gathers = [lg_gather(h) for h in range(NH)]
    live = jnp.where(c == 0, count[0], count[1]) > y * blk

    def lg_final(h):
        total = lg_s[h, y]
        for k in range(len(lg_hops)):
            arrive(lg_in.at[h, k], lg_pairs[h][k])
            total += lg_in[h, k].astype(F32)
        start = pl.multiple_of(c * cap + y * blk, blk)
        lg_all[h, :, pl.ds(start, blk)] = jnp.where(live, total, 0.0).astype(BF16)
        lg_gathers[h].far()
        lg_gathers[h].near()

    rows_of = [lax.rem(y + n_y + off, n_y) for off in (0, 1, -1, 2)]
    parity = lax.rem(z, 2)
    across_z = [lax.rem(z + n_z + 1 - 2 * lax.rem(z + k, 2), n_z) for k in range(2)]
    swap_pairs = [[sems.take() for _ in range(2)] for _ in range(NG)]

    def column_half(k):
        return pl.ds(k * half_c, half_c)

    def up_ring(g):
        if g in SWAPPED:
            at = SWAPPED.index(g)
            return ring_sum(
                lambda j, k: x_b[at, j, :, column_half(k)].astype(F32),
                lambda j, k: x_b.at[at, j, :, column_half(k)],
                lambda k: u_far.at[g, :, 0] if k is None else u_far.at[g, k, 0],
                lambda s, k: u_near.at[g, :, :, 0] if s is None else u_near.at[g, s, k, 0],
                x_b.at[at, 0:3],
                x, x_up, x_dn, x_far, lambda j: {"dp": j},
            )
        return ring_sum(
            lambda j, k: u_b[g, j, :, :, column_half(k)].astype(F32),
            lambda j, k: u_b.at[g, j, :, :, column_half(k)],
            lambda k: u_far.at[g] if k is None else u_far.at[g, k],
            lambda s, k: u_near.at[g] if s is None else u_near.at[g, s, k],
            u_b.at[g, 0:3],
            x, x_up, x_dn, x_far, lambda j: {"dp": j},
        )

    up_rings = [up_ring(g) for g in range(NG)]

    def up_part(g):
        rows = n_lat // n_x
        lhs = lat_all[pl.ds(rows_of[g] * 2, 2)].reshape(2 * n_lat, 2 * cap)
        step = 512
        for start in range(0, columns, step):
            rhs = g_v[:, :, start : start + step].reshape(2 * cap, step)
            part = dot(lhs, rhs, NN).astype(BF16)
            for k in range(2):
                for b in range(n_x):
                    at = k * n_lat + b * rows
                    u_b[g, b, k, :, start : start + step] = part[at : at + rows]
            if g in SWAPPED and (start + step) % half_c == 0:
                k = start // half_c
                ship(
                    u_b.at[g, :, 1 - parity, :, column_half(k)], u_pair.at[SWAPPED.index(g), k],
                    {"mb": across_z[k]}, swap_pairs[g][k],
                )

    def up_swap(g):
        at = SWAPPED.index(g)
        for k in range(2):
            arrive(u_pair.at[at, k], swap_pairs[g][k])
            for b in range(n_x):
                both = u_b[g, b, parity, :, column_half(k)].astype(F32) + u_pair[at, k, b].astype(F32)
                x_b[at, b, :, column_half(k)] = both.astype(BF16)

    def up_total(g):
        for k, part in enumerate(up_rings[g].total()):
            t_u[g, :, :, column_half(k)] = part.astype(BF16)
        for k in range(2):
            ship(
                t_u.at[g, 1 - parity, :, column_half(k)], t_pair.at[g, k],
                {"mb": across_z[k]}, swap_pairs[g][k],
            )

    up_hops = range(2, n_z, 2)
    up_base = list(sems.used)
    up_pairs = [sems.take() for _ in up_hops]
    to_owner = []

    def up_owner(g):
        if g in SWAPPED:
            for k, part in enumerate(up_rings[g].total()):
                f_u[rows_of[g], :, column_half(k)] = part.astype(BF16)
        for k in range(2 if g not in SWAPPED else 0):
            arrive(t_pair.at[g, k], swap_pairs[g][k])
            both = t_u[g, parity, :, column_half(k)].astype(F32) + t_pair[g, k].astype(F32)
            f_u[rows_of[g], :, column_half(k)] = both.astype(BF16)
        owner = 2 * rows_of[g] + parity
        hop = lax.rem(owner - z + n_z, n_z) // 2
        at = lax.rem(hop + n_z // 2 - 1, n_z // 2)
        slot = jnp.minimum(at, n_z // 2 - 2)
        copy = pltpu.make_async_remote_copy(
            src_ref=f_u.at[rows_of[g]], dst_ref=zr_u.at[slot],
            send_sem=send.at[up_base[0] + slot], recv_sem=recv.at[up_base[1] + slot],
            device_id={"mb": owner}, device_id_type=MESH,
        )
        pl.when(owner != z)(copy.start)
        own = pltpu.make_async_copy(f_u.at[rows_of[g]], zr_u.at[n_z // 2 - 1], save.at[2 * NH + g])
        pl.when(owner == z)(own.start)
        to_owner.append((owner, copy, own))

    def up_final():
        for d, pair in enumerate(up_pairs):
            arrive(zr_u.at[d], pair)

    cuts = [(h, lo, hi) for h in range(NH) for lo, hi in ((0, split), (split, width))]

    def down_ring(h, lo, hi):
        return ring_sum(
            lambda j, k: d_s[h, j, row_half(k, rx), lo:hi],
            lambda j, k: d_b.at[h, j, row_half(k, rx), lo:hi],
            lambda k: d_far.at[h, :, :, lo:hi] if k is None else d_far.at[h, k, :, lo:hi],
            lambda s, k: (
                d_near.at[h, :, :, :, lo:hi] if s is None else d_near.at[h, s, k, :, lo:hi]
            ),
            d_b.at[h, 0:3, :, lo:hi],
            x, x_up, x_dn, x_far, lambda j: {"dp": j},
        )

    down_rings = [down_ring(*cut) for cut in cuts]

    def down_part(i):
        h, lo, hi = cuts[i]
        lhs = lg_all[h]
        for start in range(lo, hi, 256):
            stop = min(start + 256, hi)
            part = dot(lhs, h_v[:, start:stop], NN)
            for j in range(n_x):
                rows = part[j * rx : (j + 1) * rx]
                d_s[h, j, :, start:stop] = rows
                d_b[h, j, :, start:stop] = rows.astype(BF16)

    def all_but_one(ref, i):
        h, lo, hi = cuts[i]
        return ref.at[h, 0 : n_z - 1, :, lo:hi]

    out_pairs = [sems.take() for _ in cuts]
    back_pairs = [sems.take() for _ in cuts]
    for i in range(len(cuts)):
        drains.append((all_but_one(zs_d, i), out_pairs[i]))
        drains.append((all_but_one(po_d, i), back_pairs[i]))

    def down_scatter(i):
        h, lo, hi = cuts[i]
        halves = down_rings[i].total()
        per_half = n_z // 2
        for k in range(2):
            zs_d[h, k * per_half : (k + 1) * per_half, :, lo:hi] = (
                halves[k].reshape(per_half, -1, hi - lo).astype(BF16)
            )
        zr_d[h, z, :, lo:hi] = zs_d[h, z, :, lo:hi]
        for p in z_peers:
            ship(zs_d.at[h, p, :, lo:hi], zr_d.at[h, z, :, lo:hi], {"mb": p}, out_pairs[i], False)

    def down_prefix(i):
        h, lo, hi = cuts[i]
        arrive(all_but_one(zr_d, i), out_pairs[i])
        total = zr_d[h, 0, :, lo:hi].astype(F32)
        po_d[h, 0, :, lo:hi] = total.astype(BF16)
        for p in range(1, n_z):
            total += zr_d[h, p, :, lo:hi].astype(F32)
            po_d[h, p, :, lo:hi] = total.astype(BF16)
        keep(po_d.at[h, z, :, lo:hi], rf_d.at[h, z, :, lo:hi])
        for p in z_peers:
            ship(po_d.at[h, p, :, lo:hi], rf_d.at[h, z, :, lo:hi], {"mb": p}, back_pairs[i], False)

    def down_arrive(i):
        arrive(all_but_one(rf_d, i), back_pairs[i])

    assert sems.used == [send.shape[0], recv.shape[0]], sems.used
    lat_gather.near()
    get_w[0].wait()
    get_g_other.wait()
    other_slot(0)
    get_g_own.wait()
    own_slot(0)
    get_w[1].wait()
    other_slot(1)
    pair_sum(0)
    lg_spread(0)
    lat_gather.finish(0)
    up_part(0)
    up_rings[0].far()
    up_rings[0].near()
    own_slot(1)
    pair_sum(1)
    lg_spread(1)
    lat_gather.across()
    lat_gather.finish(2)
    up_part(1)
    up_rings[1].far()
    lat_gather.finish(1)
    up_part(2)
    up_rings[0].second()
    up_rings[1].near()
    lg_final(0)
    lg_final(1)
    lat_gather.along()
    up_rings[1].second()
    up_total(0)
    lg_gathers[0].across_far()
    up_swap(2)
    up_rings[2].far()
    up_rings[2].near()
    lg_gathers[0].across()
    up_total(1)
    get_h.wait()
    lg_gathers[0].finish(0, 1, 2, 3)
    lg_gathers[1].across_far()
    down_part(0)
    down_rings[0].far()
    down_part(1)
    down_rings[1].far()
    lg_gathers[1].across()
    up_rings[2].second()
    down_rings[0].near()
    down_rings[1].near()
    up_owner(0)
    lg_gathers[1].finish(0, 1, 2, 3)
    lat_gather.across_halves()
    down_part(2)
    down_rings[2].far()
    down_part(3)
    down_rings[3].far()
    lat_gather.finish(3)
    up_part(3)
    down_rings[0].second()
    down_rings[1].second()
    down_rings[2].near()
    down_rings[3].near()
    up_owner(1)
    up_owner(2)
    down_rings[2].second()
    down_rings[3].second()
    up_rings[3].far()
    up_rings[3].near()
    down_scatter(0)
    down_scatter(1)
    down_scatter(2)
    down_scatter(3)
    up_rings[3].second()
    down_prefix(0)
    down_prefix(1)
    up_total(3)
    down_prefix(2)
    down_prefix(3)
    up_owner(3)
    down_arrive(0)
    down_arrive(1)
    down_arrive(2)
    down_arrive(3)
    up_final()
    for copy in sent:
        copy.wait_send()
    for whole, pair in drains:
        pltpu.make_async_remote_copy(
            src_ref=whole, dst_ref=whole, send_sem=pair[0], recv_sem=recv.at[0],
            device_id={"tp": partner}, device_id_type=MESH,
        ).wait_send()
    for copy in kept:
        copy.wait()
    for owner, copy, own in to_owner:
        pl.when(owner != z)(copy.wait_send)
        pl.when(owner == z)(own.wait)


def finish_kernel(up_in, down_in, up_out, down_out, up_v, down_v, up_w, down_w, load, save):
    loads = [
        pltpu.make_async_copy(src, dst, load.at[k])
        for k, (src, dst) in enumerate(((down_in, down_v), (up_in, up_v)))
    ]
    saves = [
        pltpu.make_async_copy(src, dst, save.at[k])
        for k, (src, dst) in enumerate(((down_w, down_out), (up_w, up_out)))
    ]
    for copy in loads:
        copy.start()
    loads[0].wait()
    down_w[...] = down_v[...].astype(F32).reshape(-1, down_v.shape[-1]).T
    saves[0].start()
    loads[1].wait()
    total = up_v[0].astype(F32)
    for k in range(1, up_v.shape[0]):
        total += up_v[k].astype(F32)
    up_w[...] = total
    saves[1].start()
    for copy in saves:
        copy.wait()


def local(sizes, hidden, latent, out_grad, up_weight, mb_tokens, slot_mb):
    n_z, n_y, n_x = sizes
    slot_count, cap, width = hidden.shape[1:]
    rank, columns = up_weight.shape
    n_lat = latent.shape[3]
    row_total = slot_count * cap
    rows_h = rank // NH
    rx = rows_h // n_x
    blk = cap // n_y
    rows_u = rank // n_x // n_z
    up_shape = (n_z // 2, rows_u, columns)
    down_shape = (NH, n_z, rx // n_z, width)
    in_hbm = pl.BlockSpec(memory_space=pltpu.HBM)
    both = 8 + NH + 3 * NH + 8 * NH + 2 * NG + (n_z // 2 - 1) + 2 * 2 * NH
    n_send, n_recv = both - 7 - 7 * NH + NG + 2 * NH, both + 2 * NG + 2 * 2 * NH
    up_grad, running = pl.pallas_call(
        functools.partial(kernel, n_z, n_y, n_x),
        out_shape=(
            jax.ShapeDtypeStruct(up_shape, BF16),
            jax.ShapeDtypeStruct(down_shape, BF16),
        ),
        in_specs=[in_hbm] * 6,
        out_specs=(in_hbm,) * 2,
        scratch_shapes=[
            pltpu.SMEM(mb_tokens.shape, jnp.int32),
            pltpu.SMEM(slot_mb.shape, jnp.int32),
            pltpu.VMEM((slot_count, n_lat, cap), BF16),
            pltpu.VMEM((row_total, width), BF16),
            pltpu.VMEM((slot_count, cap, columns), BF16),
            pltpu.VMEM((NH, n_x, rx, columns), BF16),
            pltpu.VMEM((2 * n_y, n_lat, row_total), BF16),
            pltpu.VMEM((NH, rows_h, cap), F32),
            pltpu.VMEM((NH, rows_h, cap), F32),
            pltpu.VMEM((NH, n_y, rows_h, blk), F32),
            pltpu.VMEM((NH, n_y, rows_h, blk), BF16),
            pltpu.VMEM((NH, 3, rows_h, blk), BF16),
            pltpu.VMEM((NH, rows_h, row_total), BF16),
            pltpu.VMEM((NH, n_x, rx, width), F32),
            pltpu.VMEM((NH, n_x, rx, width), BF16),
            pltpu.VMEM((NH, 2, rx // 2, width), BF16),
            pltpu.VMEM((NH, 2, 2, rx // 2, width), BF16),
            pltpu.VMEM(down_shape, BF16),
            pltpu.VMEM(down_shape, BF16),
            pltpu.VMEM(down_shape, BF16),
            pltpu.VMEM((NG, n_x, 2, rows_u, columns), BF16),
            pltpu.VMEM((len(SWAPPED), 2, n_x, rows_u, columns // 2), BF16),
            pltpu.VMEM((len(SWAPPED), n_x, rows_u, columns), BF16),
            pltpu.VMEM((NG, 2, 2, rows_u, columns // 2), BF16),
            pltpu.VMEM((NG, 2, 2, 2, rows_u, columns // 2), BF16),
            pltpu.VMEM((NG, 2, rows_u, columns), BF16),
            pltpu.VMEM((NG, 2, rows_u, columns // 2), BF16),
            pltpu.VMEM((n_y, rows_u, columns), BF16),
            pltpu.SemaphoreType.DMA((6 + NH,)),
            pltpu.SemaphoreType.DMA((2 * NH + NG,)),
            pltpu.SemaphoreType.DMA((n_send,)),
            pltpu.SemaphoreType.DMA((n_recv,)),
        ],
        compiler_params=pltpu.CompilerParams(
            collective_id=0, has_side_effects=True, vmem_limit_bytes=66_400_000
        ),
    )(
        hidden.reshape(row_total, width),
        latent[0].swapaxes(1, 2),
        out_grad.reshape(slot_count, cap, columns),
        up_weight.reshape(n_x, NH, rx, columns),
        mb_tokens,
        slot_mb,
    )
    up_grad, running = pl.pallas_call(
        finish_kernel,
        out_shape=(
            jax.ShapeDtypeStruct((rows_u, columns), F32),
            jax.ShapeDtypeStruct((width, rank // n_x), F32),
        ),
        in_specs=[in_hbm] * 2,
        out_specs=(in_hbm,) * 2,
        scratch_shapes=[
            pltpu.VMEM(up_shape, BF16),
            pltpu.VMEM(down_shape, BF16),
            pltpu.VMEM((rows_u, columns), F32),
            pltpu.VMEM((width, rank // n_x), F32),
            pltpu.SemaphoreType.DMA((2,)),
            pltpu.SemaphoreType.DMA((2,)),
        ],
        compiler_params=pltpu.CompilerParams(vmem_limit_bytes=66_400_000),
    )(up_grad, running)
    return up_grad, running[None]


def solution(mesh):
    sizes = (mesh.shape["mb"], mesh.shape["tp"] // 2, mesh.shape["dp"])
    return jax.shard_map(
        functools.partial(local, sizes),
        mesh=mesh,
        in_specs=(
            P("dp", "mb", None, "tp"),
            P("dp", "mb", None, "tp"),
            P("dp", "mb", None, "tp"),
            P(None, "tp"),
            P("dp", None),
            P("dp", "mb"),
        ),
        out_specs=(P(("mb", "dp"), "tp"), P("mb", "tp", "dp")),
        check_vma=False,
    )
```
